32 devices in a mesh: seq: 16 (over z, y, core), mp: 2 (over x).
Axes of the slice: x: 2, y: 2, z: 4, core: 2. Of those that a mesh axis runs over, the one named last changes fastest.
Arguments:
- stream: bfloat16 [2048, 8192], P('seq', 'mp'), may hold values from -17 to 17
- norm_gain: float32 [8192], P('mp'), may hold values from 0.5 to 1.5
- short_outer: bfloat16 [2048, 8192], P('seq', 'mp'), may hold values from -4 to 4
- short_inner: bfloat16 [2048, 8192], P('seq', 'mp'), may hold values from -4 to 4
- short_filter: bfloat16 [128, 8192], P(None, 'mp'), may hold values from -0.5 to 0.5
- long_outer: bfloat16 [2048, 8192], P('seq', 'mp'), may hold values from -4 to 4
- long_inner: bfloat16 [2048, 8192], P('seq', 'mp'), may hold values from -4 to 4
- long_decay: float32 [8192], P('mp'), may hold values from 1e-06 to 0.03
- query_heads: bfloat16 [2048, 8192], P('seq', 'mp'), may hold values from -6 to 6
- key_heads: bfloat16 [2048, 8192], P('seq', 'mp'), may hold values from -6 to 6
Outputs:
- long_mixed: bfloat16 [2048, 8192], P('seq', 'mp')
- attended: bfloat16 [2048, 8192], P('seq', 'mp')
The draws below stay inside these ranges and needn't reach their ends.
All inputs are finite; a program needn't handle non-finite values.
Results may differ from the reference program's by a relative error of at most 0.013.
Values may be sent and summed in bfloat16 or wider, within the bound.
A program may use at most 64 MiB of HBM per device.

```python
import math
import jax
import jax.numpy as jnp
from jax import lax

D = 8192
HEADS = 64
HEAD_DIM = 128
TAPS = 128
TOK_DEV = 128
SEQ_LEN = 2048
N_SEQ = 16


def draw_stream(key, part):
    shape = (SEQ_LEN, D // 128, 128)
    base = jnp.clip(jax.random.normal(jax.random.fold_in(key, 11), shape, jnp.float32), -4.0, 4.0)
    levels = jnp.exp(jax.random.uniform(jax.random.fold_in(key, 13), (SEQ_LEN, D // 128, 1), jnp.float32, -1.4, 1.4))
    return (base * levels).reshape(SEQ_LEN, D).astype(jnp.bfloat16)


def draw_long_decay(key, part):
    upper = math.log(0.03)
    return jnp.exp(jax.random.uniform(jax.random.fold_in(key, 41), (D,), jnp.float32, math.log(1e-06), upper))


def draw_heads(key, salt):
    drawn = jnp.clip(jax.random.normal(jax.random.fold_in(key, salt), (SEQ_LEN, D), jnp.float32), -6.0, 6.0)
    return drawn


def draw_query_heads(key, part):
    return draw_heads(key, 31).astype(jnp.bfloat16)


def draw_key_heads(key, part):
    return draw_heads(key, 32).astype(jnp.bfloat16)


def block_scale(rng, extent, split, low, high):
    loudness, own = 1.0, jax.random.fold_in(rng, 6)
    for axis_at, parts in split:
        heights = jnp.exp(jax.random.uniform(jax.random.fold_in(own, axis_at), (parts,), jnp.float32, low / len(split), high / len(split)))
        loudness = loudness * jnp.repeat(heights, extent[axis_at] // parts).reshape([-1 if axis == axis_at else 1 for axis in range(len(extent))])
    return loudness


def normal_values(key, extent, width, most, cuts=(), kind=jnp.bfloat16):
    values = width * jax.random.normal(key, extent, jnp.float32)
    if cuts:
        values = values * block_scale(key, extent, cuts, -0.22, 0.18)
    return jnp.clip(values, -most, most).astype(kind)


def setup_inputs(seed: int = 0) -> dict:
    key_list = jax.random.split(jax.random.key(seed), 11)
    stream = draw_stream(jax.random.fold_in(key_list[10], 71), 0)
    norm_gain = jnp.clip(1.0 + 0.1 * jax.random.normal(key_list[1], (D,), jnp.float32), 0.5, 1.5)
    short_outer = normal_values(key_list[2], (SEQ_LEN, D), 1.0, 4.0, ((0, 16), (1, 2)))
    short_inner = normal_values(key_list[3], (SEQ_LEN, D), 1.0, 4.0, ((0, 16), (1, 2)))
    short_filter = normal_values(key_list[4], (TAPS, D), TAPS ** -0.5, 0.5, ((1, 2),))
    long_outer = normal_values(key_list[5], (SEQ_LEN, D), 1.0, 4.0, ((0, 16), (1, 2)))
    long_inner = normal_values(key_list[6], (SEQ_LEN, D), 1.0, 4.0, ((0, 16), (1, 2)))
    long_decay = draw_long_decay(jax.random.fold_in(key_list[10], 71), 0)
    query_heads = draw_query_heads(jax.random.fold_in(key_list[10], 71), 0)
    key_heads = draw_key_heads(jax.random.fold_in(key_list[10], 71), 0)
    return {"stream": stream, "norm_gain": norm_gain, "short_outer": short_outer, "short_inner": short_inner, "short_filter": short_filter, "long_outer": long_outer, "long_inner": long_inner, "long_decay": long_decay, "query_heads": query_heads, "key_heads": key_heads}


def pair_combine(first_pair, second_pair):
    return (first_pair[0] * second_pair[0], second_pair[0] * first_pair[1] + second_pair[1])

def reference(stream, norm_gain, short_outer, short_inner, short_filter, long_outer, long_inner, long_decay, query_heads, key_heads):
    rates = jnp.exp(-long_decay)
    scales = jnp.sqrt(-jnp.expm1(-2.0 * long_decay))
    filt = short_filter.astype(jnp.float32)

    def blocked(array):
        return array.reshape(N_SEQ, TOK_DEV, D)
    inputs = (jnp.arange(N_SEQ, dtype=jnp.int32), blocked(stream), blocked(short_outer), blocked(short_inner), blocked(long_outer), blocked(long_inner), blocked(query_heads), blocked(key_heads))

    def block_step(carry, pieces):
        tail, state, prev_keys, prev_values = carry
        block_index, x_blk, s_outer, s_inner, l_outer, l_inner, q_blk, k_blk = pieces
        x_float = x_blk.astype(jnp.float32)
        mean_square = lax.optimization_barrier(jnp.mean(x_float * x_float, axis=1, keepdims=True))
        normed = x_float * norm_gain / jnp.sqrt(mean_square + 0.5)
        short_in = (s_inner.astype(jnp.float32) * normed).astype(jnp.bfloat16)
        extended = jnp.concatenate([tail, short_in], axis=0).astype(jnp.float32)

        def tap_step(j, acc):
            start = (TAPS - 1 - j).astype(jnp.int32)
            window = lax.dynamic_slice_in_dim(extended, start, TOK_DEV, 0)
            return acc + lax.dynamic_slice_in_dim(filt, j.astype(jnp.int32), 1, 0) * window
        short_conv = lax.fori_loop(0, TAPS, tap_step, jnp.zeros((TOK_DEV, D), jnp.float32))
        long_in = (l_inner.astype(jnp.float32) * s_outer.astype(jnp.float32) * short_conv).astype(jnp.bfloat16)
        factors = jnp.broadcast_to(rates, long_in.shape)
        powers, states = lax.associative_scan(pair_combine, (factors, long_in.astype(jnp.float32)), axis=0)
        states = states + powers * state
        long_mixed = (l_outer.astype(jnp.float32) * (states * scales)).astype(jnp.bfloat16)
        query = q_blk.astype(jnp.float32).reshape(TOK_DEV, HEADS, HEAD_DIM)
        keys = jnp.concatenate([prev_keys, k_blk], axis=0).astype(jnp.float32).reshape(2 * TOK_DEV, HEADS, HEAD_DIM)
        values = jnp.concatenate([prev_values, long_mixed], axis=0).astype(jnp.float32).reshape(2 * TOK_DEV, HEADS, HEAD_DIM)
        scores = jnp.einsum('thd,shd->hts', query, keys) * HEAD_DIM ** (-0.5)
        row_pos = jnp.arange(TOK_DEV, dtype=jnp.int32)[:, None]
        col_pos = jnp.arange(2 * TOK_DEV, dtype=jnp.int32)[None, :]
        valid = (col_pos <= row_pos + TOK_DEV) & ((col_pos >= TOK_DEV) | (block_index > 0))
        scores = jnp.where(valid[None], scores, -1e+30)
        weights = jax.nn.softmax(scores, axis=-1).astype(jnp.bfloat16)
        result = jnp.einsum('hts,shd->thd', weights.astype(jnp.float32), values)
        attended = result.reshape(TOK_DEV, D).astype(jnp.bfloat16)
        new_carry = (short_in[TOK_DEV - (TAPS - 1):], states[-1], k_blk, long_mixed)
        return (new_carry, (long_mixed, attended))
    start_carry = (jnp.zeros((TAPS - 1, D), jnp.bfloat16), jnp.zeros((D,), jnp.float32), jnp.zeros((TOK_DEV, D), jnp.bfloat16), jnp.zeros((TOK_DEV, D), jnp.bfloat16))
    _, outputs = lax.scan(block_step, start_carry, inputs)
    long_mixed = outputs[0].reshape(SEQ_LEN, D)
    attended = outputs[1].reshape(SEQ_LEN, D)
    return (long_mixed, attended)
```

```python
import functools

import jax
import jax.numpy as jnp
import numpy as np
from jax import lax
from jax.experimental import pallas as pl
from jax.experimental.pallas import tpu as pltpu
from jax.sharding import PartitionSpec as P

HEAD_DIM = 128
CHUNKS = 4
PAIR = 2
EARLY = 2
STORES = 2
TILE = 256
MESH = pl.DeviceIdType.MESH


def wave(frequency, place, rows):
    shift = jnp.where(frequency >= rows, rows, 0)
    index = lax.rem((2 * lax.rem(frequency, rows) + 1) * place + shift, 4 * rows)
    return jnp.cos(index.astype(jnp.float32) * (np.pi / (2 * rows)))


def dot(a, b):
    return jnp.dot(a, b, preferred_element_type=jnp.float32)


def kernel(
    n,
    mp,
    channels,
    gain_hbm,
    decay_hbm,
    stream_hbm,
    souter_hbm,
    sinner_hbm,
    filt_hbm,
    louter_hbm,
    linner_hbm,
    query_hbm,
    key_hbm,
    mixed,
    attended,
    vectors,
    blocks,
    fwd,
    inv,
    keys,
    values,
    ext,
    power,
    inv_power,
    cum,
    spectrum,
    weights,
    squares,
    squares_in,
    own_state,
    pair_state,
    group_state,
    next_state,
    carry_in,
    states,
    load_sem,
    key_sem,
    sq_send,
    sq_recv,
    k_send,
    k_recv,
    t_send,
    t_recv,
    v_send,
    v_recv,
    p_send,
    p_recv,
    q_send,
    q_recv,
    e_send,
    e_recv,
):
    gain_ref, decay_ref = vectors.at[0], vectors.at[1]
    stream, sinner, filt, souter, linner, louter, query = (blocks.at[i] for i in range(7))
    me = lax.axis_index("seq")
    col = lax.axis_index("mp")
    rows, width = stream.shape
    wide = width // CHUNKS
    tiles = wide // TILE
    heads = wide // HEAD_DIM
    has_next = me < n - 1
    has_prev = me > 0
    groups = n // PAIR
    group = me // PAIR
    leads = lax.rem(me, PAIR) == 0
    follows = lax.rem(me, PAIR) != 0
    own = pl.ds(rows, rows)
    before = pl.ds(0, rows)

    barrier = pltpu.get_barrier_semaphore()

    def greet(target):
        pl.semaphore_signal(barrier, inc=1, device_id={"seq": target}, device_id_type=MESH)

    @pl.when(has_next)
    def _():
        greet(me + 1)

    @pl.when(has_prev)
    def _():
        greet(me - 1)

    @pl.when(leads)
    def _():
        def greet_leader(k, _):
            greet(lax.rem(me + PAIR * k, n))
            return 0

        lax.fori_loop(1, groups, greet_leader, 0)

    for k in range(1, mp):
        pl.semaphore_signal(
            barrier, inc=1, device_id={"mp": lax.rem(col + k, mp)}, device_id_type=MESH
        )

    def load(source, target, sem):
        copy = pltpu.make_async_copy(source, target, sem)
        copy.start()

    def landed(buffer, sem):
        pltpu.make_async_copy(buffer, buffer, sem).wait()

    def load_key(c, sem):
        load(key_hbm.at[:, pl.ds(c * wide, wide)], keys.at[c, own], sem)

    for c in range(EARLY):
        load_key(c, key_sem.at[c])
    load(stream_hbm, stream, load_sem.at[0])
    load(sinner_hbm, sinner, load_sem.at[1])
    load(gain_hbm, gain_ref, load_sem.at[2])
    load(decay_hbm, decay_ref, load_sem.at[2])

    def to_next(buffer, c, send, recv):
        return pltpu.make_async_remote_copy(
            src_ref=buffer.at[c, own],
            dst_ref=buffer.at[c, before],
            send_sem=send.at[0],
            recv_sem=recv.at[c],
            device_id={"seq": lax.rem(me + 1, n)},
            device_id_type=MESH,
        )

    k_copies = [to_next(keys, c, k_send, k_recv) for c in range(CHUNKS)]
    t_copies = [to_next(ext, c, t_send, t_recv) for c in range(CHUNKS)]
    v_copies = [to_next(values, c, v_send, v_recv) for c in range(CHUNKS)]

    @pl.when(me == 0)
    def _():
        for c in range(CHUNKS):
            keys[c, :rows, :] = jnp.zeros((rows, wide), keys.dtype)
            values[c, :rows, :] = jnp.zeros((rows, wide), values.dtype)
            ext[c, :rows, :] = jnp.zeros((rows, wide), ext.dtype)

    greeted = has_next.astype(jnp.int32) + has_prev.astype(jnp.int32) + mp - 1
    pl.semaphore_wait(barrier, jnp.where(leads, greeted + groups - 1, greeted))
    for c in range(EARLY):
        landed(keys.at[c, own], key_sem.at[c])

        @pl.when(has_next)
        def _(c=c):
            k_copies[c].start()

    load(filt_hbm, filt, load_sem.at[3])
    for c in range(EARLY, CHUNKS):
        load_key(c, key_sem.at[EARLY])
    load(souter_hbm, souter, load_sem.at[4])
    load(linner_hbm, linner, load_sem.at[4])
    load(query_hbm, query, load_sem.at[5])
    load(louter_hbm, louter, load_sem.at[6])
    landed(stream, load_sem.at[0])

    def square(i, acc):
        x = stream[:, pl.ds(pl.multiple_of(i * 128, 128), 128)].astype(jnp.float32)
        return acc + x * x

    total = lax.fori_loop(
        0, width // 128, square, jnp.zeros((rows, 128), jnp.float32), unroll=4
    )
    squares[...] = jnp.sum(total.T.reshape(128 // 8, 8, rows), axis=0)
    sq_copies = [
        pltpu.make_async_remote_copy(
            src_ref=squares,
            dst_ref=squares_in.at[k - 1],
            send_sem=sq_send.at[k - 1],
            recv_sem=sq_recv.at[k - 1],
            device_id={"mp": lax.rem(col + k, mp)},
            device_id_type=MESH,
        )
        for k in range(1, mp)
    ]
    for copy in sq_copies:
        copy.start()
    landed(sinner, load_sem.at[1])
    landed(vectors, load_sem.at[2])
    total = squares[...]
    for k, copy in enumerate(sq_copies):
        copy.wait_recv()
        total = total + squares_in[k]
    mean_square = jnp.sum(total, axis=0, keepdims=True) / channels
    norm = jnp.broadcast_to(1.0 / jnp.sqrt(mean_square + 0.5), (128, rows)).T
    norm = jnp.concatenate([norm] * (TILE // 128), axis=1)

    for c in range(CHUNKS):

        def short(i, _, c=c):
            cols = pl.ds(pl.multiple_of(c * wide + i * TILE, TILE), TILE)
            x = stream[:, cols].astype(jnp.float32) * gain_ref[:, cols] * norm
            ext[c, own, pl.ds(pl.multiple_of(i * TILE, TILE), TILE)] = (
                sinner[:, cols].astype(jnp.float32) * x
            ).astype(jnp.bfloat16)
            return 0

        lax.fori_loop(0, tiles, short, 0)

        @pl.when(has_next)
        def _(c=c):
            t_copies[c].start()

    landed(keys.at[pl.ds(EARLY, CHUNKS - EARLY), own], key_sem.at[EARLY])

    @pl.when(has_next)
    def _():
        for c in range(EARLY, CHUNKS):
            k_copies[c].start()

    full = (2 * rows, 2 * rows)
    fwd[...] = wave(
        lax.broadcasted_iota(jnp.int32, full, 0), lax.broadcasted_iota(jnp.int32, full, 1), rows
    ).astype(jnp.bfloat16)
    half = (rows, 2 * rows)
    inv[...] = (
        wave(
            lax.broadcasted_iota(jnp.int32, half, 1),
            lax.broadcasted_iota(jnp.int32, half, 0) + rows,
            rows,
        )
        / rows
    ).astype(jnp.bfloat16)

    def spectra(i, _):
        cols = pl.ds(pl.multiple_of(i * TILE, TILE), TILE)
        spectrum[:, cols] = dot(fwd[:, :rows], filt[:, cols])
        return 0

    landed(filt, load_sem.at[3])
    lax.fori_loop(0, width // TILE, spectra, 0)

    step = lax.broadcasted_iota(jnp.int32, (rows, TILE), 0).astype(jnp.float32)

    def powers(i, _):
        cols = pl.ds(pl.multiple_of(i * TILE, TILE), TILE)
        exponent = step * decay_ref[:, cols]
        power[:, cols] = jnp.exp(-exponent)
        inv_power[:, cols] = jnp.exp(exponent)
        return 0

    lax.fori_loop(0, width // TILE, powers, 0)
    landed(blocks.at[pl.ds(3, 2)], load_sem.at[4])
    row = lax.broadcasted_iota(jnp.int32, (rows, 2 * rows), 0)
    column = lax.broadcasted_iota(jnp.int32, (rows, 2 * rows), 1)
    lower = (jnp.where(column >= rows, column - rows, column) <= row).astype(
        jnp.float32
    ).astype(jnp.bfloat16)

    def state_copy(c, target):
        return pltpu.make_async_remote_copy(
            src_ref=group_state.at[c],
            dst_ref=states.at[c, group],
            send_sem=e_send.at[target],
            recv_sem=e_recv.at[c, group],
            device_id={"seq": lax.rem(target * PAIR, n)},
            device_id_type=MESH,
        )

    p_copies = [
        pltpu.make_async_remote_copy(
            src_ref=own_state.at[c],
            dst_ref=pair_state.at[c],
            send_sem=p_send.at[0],
            recv_sem=p_recv.at[c],
            device_id={"seq": lax.rem(me + n - 1, n)},
            device_id_type=MESH,
        )
        for c in range(CHUNKS)
    ]
    q_copies = [
        pltpu.make_async_remote_copy(
            src_ref=next_state.at[c],
            dst_ref=carry_in.at[c],
            send_sem=q_send.at[0],
            recv_sem=q_recv.at[c],
            device_id={"seq": lax.rem(me + 1, n)},
            device_id_type=MESH,
        )
        for c in range(CHUNKS)
    ]

    for c in range(CHUNKS):

        @pl.when(has_prev)
        def _(c=c):
            t_copies[c].wait_recv()

        def mix(i, _, c=c):
            here = pl.ds(pl.multiple_of(i * TILE, TILE), TILE)
            cols = pl.ds(pl.multiple_of(c * wide + i * TILE, TILE), TILE)
            x = dot(fwd[...], ext[c, :, here])
            x_re, x_im = x[:rows], x[rows:]
            h_re, h_im = spectrum[:rows, cols], spectrum[rows:, cols]
            y = jnp.concatenate(
                [x_re * h_re - x_im * h_im, x_re * h_im + x_im * h_re], axis=0
            ).astype(jnp.bfloat16)
            conv = dot(inv[...], y)
            long_in = (
                linner[:, cols].astype(jnp.float32) * souter[:, cols].astype(jnp.float32) * conv
            ).astype(jnp.bfloat16)
            v = long_in.astype(jnp.float32) * inv_power[:, cols]
            high = v.astype(jnp.bfloat16)
            low = (v - high.astype(jnp.float32)).astype(jnp.bfloat16)
            sums = dot(lower, jnp.concatenate([high, low], axis=0))
            cum[:, cols] = sums
            own_state[c, :, here] = sums[rows - 1 :] * power[rows - 1 :, cols]
            return 0

        lax.fori_loop(0, tiles, mix, 0)

        @pl.when(follows)
        def _(c=c):
            p_copies[c].start()

        @pl.when(leads)
        def _(c=c):
            p_copies[c].wait_recv()
            rate = decay_ref[:, pl.ds(c * wide, wide)]
            group_state[c] = own_state[c] * jnp.exp(-rate * rows) + pair_state[c]

            def send_state(target, _, c=c):
                state_copy(c, target).start()
                return 0

            lax.fori_loop(group + 1, groups, send_state, 0)

    landed(louter, load_sem.at[6])
    for c in range(CHUNKS):
        chunk = pl.ds(c * wide, wide)
        rate = decay_ref[:, chunk]

        @pl.when(leads)
        def _(c=c, rate=rate):
            over_group = jnp.exp(-rate * (rows * PAIR))

            def arrive(j, state):
                pltpu.make_async_remote_copy(
                    src_ref=group_state.at[c],
                    dst_ref=states.at[c, j],
                    send_sem=e_send.at[group],
                    recv_sem=e_recv.at[c, j],
                    device_id={"seq": j * PAIR},
                    device_id_type=MESH,
                ).wait_recv()
                return state * over_group + states[c, j]

            state = lax.fori_loop(0, group, arrive, jnp.zeros((1, wide), jnp.float32))
            next_state[c] = state * jnp.exp(-rate * rows) + own_state[c]
            q_copies[c].start()
            carry_in[c] = state

        @pl.when(follows)
        def _(c=c):
            q_copies[c].wait_recv()

        carried = carry_in[c]
        carried = carried * jnp.exp(-rate)
        z = 2.0 * rate
        scale = jnp.sqrt(jnp.tanh(0.5 * z) * (1.0 + jnp.exp(-z)))
        for i in range(tiles):
            here = pl.ds(i * TILE, TILE)
            cols = pl.ds(c * wide + i * TILE, TILE)
            part = slice(i * TILE, (i + 1) * TILE)
            conv = (cum[:, cols] + carried[:, part]) * power[:, cols]
            out = (
                louter[:, cols].astype(jnp.float32) * (conv * scale[:, part])
            ).astype(jnp.bfloat16)
            values[c, own, here] = out
            mixed[:, cols] = out

        @pl.when(has_next)
        def _(c=c):
            v_copies[c].start()

    landed(query, load_sem.at[5])
    valid = (column <= row + rows) & ((column >= rows) | has_prev)
    for c in range(CHUNKS):

        @pl.when(has_prev)
        def _(c=c):
            k_copies[c].wait_recv()

        def score(h, _, c=c):
            here = pl.ds(pl.multiple_of(h * HEAD_DIM, HEAD_DIM), HEAD_DIM)
            cols = pl.ds(pl.multiple_of(c * wide + h * HEAD_DIM, HEAD_DIM), HEAD_DIM)
            s = lax.dot_general(
                query[:, cols],
                keys[c, :, here],
                (((1,), (1,)), ((), ())),
                preferred_element_type=jnp.float32,
            ) * HEAD_DIM ** (-0.5)
            s = jnp.where(valid, s, -1e30)
            e = jnp.exp(s - jnp.max(s, axis=1, keepdims=True))
            e = e * (1.0 / jnp.sum(e, axis=1, keepdims=True))
            weights[c, h] = e.astype(jnp.bfloat16)
            return 0

        lax.fori_loop(0, heads, score, 0, unroll=2)

    for c in range(CHUNKS):

        @pl.when(has_prev)
        def _(c=c):
            v_copies[c].wait_recv()

        def gather(h, _, c=c):
            here = pl.ds(pl.multiple_of(h * HEAD_DIM, HEAD_DIM), HEAD_DIM)
            cols = pl.ds(pl.multiple_of(c * wide + h * HEAD_DIM, HEAD_DIM), HEAD_DIM)
            attended[:, cols] = dot(weights[c, h], values[c, :, here]).astype(jnp.bfloat16)
            return 0

        lax.fori_loop(0, heads, gather, 0, unroll=8)

    for copy in sq_copies:
        copy.wait_send()

    def sent(buffer, sem):
        pltpu.make_async_copy(buffer, buffer, sem).wait()

    @pl.when(follows)
    def _():
        sent(own_state, p_send.at[0])

    @pl.when(leads)
    def _():
        sent(next_state, q_send.at[0])

        def all_sent(target, _):
            sent(group_state, e_send.at[target])
            return 0

        lax.fori_loop(group + 1, groups, all_sent, 0)

    @pl.when(has_next)
    def _():
        sent(keys.at[:, own], k_send.at[0])
        sent(ext.at[:, own], t_send.at[0])
        sent(values.at[:, own], v_send.at[0])


def store(mixed, attended, mixed_hbm, attended_hbm, sem):
    rows = mixed.shape[0]
    parts = [pl.ds(i * rows // STORES, rows // STORES) for i in range(STORES)]
    copies = [
        pltpu.make_async_copy(source.at[part], target.at[part], sem.at[k, i])
        for k, (source, target) in enumerate([(mixed, mixed_hbm), (attended, attended_hbm)])
        for i, part in enumerate(parts)
    ]
    for copy in copies:
        copy.start()
    for copy in copies:
        copy.wait()


def on_device(
    n,
    mp,
    stream,
    norm_gain,
    short_outer,
    short_inner,
    short_filter,
    long_outer,
    long_inner,
    long_decay,
    query_heads,
    key_heads,
):
    rows, width = stream.shape
    wide = width // CHUNKS
    bf16, f32 = jnp.bfloat16, jnp.float32
    anywhere = pl.BlockSpec(memory_space=pltpu.HBM)
    vmem = pl.BlockSpec(memory_space=pltpu.VMEM)
    dma = pltpu.SemaphoreType.DMA

    def in_hbm(array):
        return pltpu.with_memory_space_constraint(array, pltpu.HBM)

    mixed, attended = pl.pallas_call(
        functools.partial(kernel, n, mp, float(width * mp)),
        out_shape=[jax.ShapeDtypeStruct((rows, width), bf16)] * 2,
        in_specs=[anywhere] * 10,
        out_specs=[vmem] * 2,
        scratch_shapes=[
            pltpu.VMEM((2, 1, width), f32),
            pltpu.VMEM((7, rows, width), bf16),
            pltpu.VMEM((2 * rows, 2 * rows), bf16),
            pltpu.VMEM((rows, 2 * rows), bf16),
        ]
        + [pltpu.VMEM((CHUNKS, 2 * rows, wide), bf16)] * 3
        + [pltpu.VMEM((rows, width), f32)] * 3
        + [
            pltpu.VMEM((2 * rows, width), f32),
            pltpu.VMEM((CHUNKS, wide // HEAD_DIM, rows, 2 * rows), bf16),
            pltpu.VMEM((8, rows), f32),
            pltpu.VMEM((mp - 1, 8, rows), f32),
        ]
        + [pltpu.VMEM((CHUNKS, 1, wide), f32)] * 5
        + [
            pltpu.VMEM((CHUNKS, n // PAIR, 1, wide), f32),
            dma((7,)),
            dma((EARLY + 1,)),
            dma((mp - 1,)),
            dma((mp - 1,)),
        ]
        + [dma((1,)), dma((CHUNKS,))] * 5
        + [dma((n // PAIR,)), dma((CHUNKS, n // PAIR))],
        compiler_params=pltpu.CompilerParams(
            collective_id=0, has_side_effects=True, vmem_limit_bytes=51 * 1024 * 1024
        ),
    )(
        in_hbm(norm_gain.reshape(1, width)),
        in_hbm(long_decay.reshape(1, width)),
        stream,
        short_outer,
        short_inner,
        short_filter,
        long_outer,
        long_inner,
        query_heads,
        key_heads,
    )
    return pl.pallas_call(
        store,
        out_shape=[jax.ShapeDtypeStruct((rows, width), bf16)] * 2,
        in_specs=[vmem] * 2,
        out_specs=[anywhere] * 2,
        scratch_shapes=[dma((2, STORES))],
        compiler_params=pltpu.CompilerParams(vmem_limit_bytes=1024 * 1024),
    )(mixed, attended)


def solution(mesh):
    return jax.shard_map(
        functools.partial(on_device, mesh.shape["seq"], mesh.shape["mp"]),
        mesh=mesh,
        in_specs=(
            P("seq", "mp"),
            P("mp"),
            P("seq", "mp"),
            P("seq", "mp"),
            P(None, "mp"),
            P("seq", "mp"),
            P("seq", "mp"),
            P("mp"),
            P("seq", "mp"),
            P("seq", "mp"),
        ),
        out_specs=(P("seq", "mp"), P("seq", "mp")),
        check_vma=False,
    )
```

```python
import functools

import jax
import jax.numpy as jnp
import numpy as np
from jax import lax
from jax.experimental import pallas as pl
from jax.experimental.pallas import tpu as pltpu
from jax.sharding import PartitionSpec as P

HEAD_DIM = 128
CHUNKS = 4
HALF = CHUNKS // 2
LENT = CHUNKS - 1
GROUP = 4
TILE = 256
STORES = 2
MESH = pl.DeviceIdType.MESH


def wave(frequency, place, rows):
    shift = np.where(frequency >= rows, rows, 0)
    index = ((2 * (frequency % rows) + 1) * place + shift) % (4 * rows)
    return np.cos(index * (np.pi / (2 * rows)))


def waves_of(rows):
    every = np.arange(2 * rows)
    fwd = wave(every[:, None], every[None, :], rows)
    inv = wave(every[None, :], every[:rows, None] + rows, rows) / rows
    return np.concatenate([fwd, inv], axis=0)


def dot(a, b):
    return jnp.dot(a, b, preferred_element_type=jnp.float32)


def dot_nt(a, b):
    return lax.dot_general(a, b, (((1,), (1,)), ((), ())), preferred_element_type=jnp.float32)


def dot_tn(a, b):
    return lax.dot_general(a, b, (((0,), (0,)), ((), ())), preferred_element_type=jnp.float32)


def kernel(
    n,
    mp,
    channels,
    gain_hbm,
    decay_hbm,
    waves_hbm,
    stream_hbm,
    souter_hbm,
    sinner_hbm,
    filt_hbm,
    louter_hbm,
    linner_hbm,
    query_hbm,
    key_hbm,
    mixed,
    attended,
    vectors,
    blocks,
    waves,
    keys,
    values,
    ext,
    relayed,
    next_query,
    lent,
    own_part,
    shares,
    power,
    inv_power,
    cum,
    spectrum,
    weights,
    lent_weights,
    stats,
    stats_in,
    squares,
    squares_in,
    own_state,
    member_state,
    pair_state,
    before_state,
    group_state,
    next_state,
    carry_in,
    states,
    load_sem,
    key_sem,
    sq_send,
    sq_recv,
    k_send,
    k_recv,
    t_send,
    t_recv,
    v_send,
    v_recv,
    r_send,
    r_recv,
    p_send,
    p_recv,
    q_send,
    q_recv,
    g_send,
    g_recv,
    e_send,
    e_recv,
    lend_send,
    lend_recv,
):
    gain_ref, decay_ref = vectors.at[0], vectors.at[1]
    stream, sinner, filt, souter, linner, louter, query = (blocks.at[i] for i in range(7))
    me = lax.axis_index("seq")
    col = lax.axis_index("mp")
    rows, width = stream.shape
    fwd, inv = waves.at[pl.ds(0, 2 * rows)], waves.at[pl.ds(2 * rows, rows)]
    wide = width // CHUNKS
    tiles = wide // TILE
    heads = wide // HEAD_DIM
    has_next = me < n - 1
    has_prev = me > 0
    groups = n // GROUP
    group = me // GROUP
    role = lax.rem(me, GROUP)
    later = groups - 1 - group
    first = role == 0
    lends = role == 1
    borrows = role == 2
    relays = jnp.logical_and(role == 3, later > 0)
    forwards = jnp.logical_and(lends, later > 0)
    even = lax.rem(me, 2) == 0
    own = pl.ds(rows, rows)
    before = pl.ds(0, rows)

    def seq(target):
        return {"seq": lax.rem(target + n, n)}

    barrier = pltpu.get_barrier_semaphore()

    def greet(target, when):
        @pl.when(when)
        def _():
            pl.semaphore_signal(barrier, inc=1, device_id=seq(target), device_id_type=MESH)

    greet(me + 1, has_next)
    greet(me - 1, has_prev)
    greet(me - 2, borrows)
    greet(me + 2, forwards)
    greet(me - 3, jnp.logical_and(first, group > 0))

    @pl.when(even)
    def _():
        def greet_earlier(j, _):
            pl.semaphore_signal(
                barrier, inc=1, device_id=seq(j * GROUP + 2), device_id_type=MESH
            )
            return 0

        lax.fori_loop(0, group, greet_earlier, 0)

    greeted = has_next.astype(jnp.int32) + has_prev.astype(jnp.int32) + mp - 1
    greeted += jnp.where(borrows, 2 * later, 0)
    greeted += (first | relays | forwards).astype(jnp.int32)

    for k in range(1, mp):
        pl.semaphore_signal(
            barrier, inc=1, device_id={"mp": lax.rem(col + k, mp)}, device_id_type=MESH
        )

    def load(source, target, sem):
        pltpu.make_async_copy(source, target, sem).start()

    def landed(buffer, sem):
        pltpu.make_async_copy(buffer, buffer, sem).wait()

    def load_key(c, sem):
        load(key_hbm.at[:, pl.ds(c * wide, wide)], keys.at[c, own], sem)

    others = [c for c in range(1, CHUNKS) if c != HALF]
    last = pl.ds(LENT * wide, wide)
    rest = pl.ds(0, LENT * wide)
    load(query_hbm.at[:, last], query.at[:, last], load_sem.at[6])
    load_key(0, key_sem.at[0])
    load_key(HALF, key_sem.at[1])
    load(stream_hbm, stream, load_sem.at[0])
    load(gain_hbm, gain_ref, load_sem.at[2])
    load(decay_hbm, decay_ref, load_sem.at[2])
    load(waves_hbm, waves, load_sem.at[3])
    load(filt_hbm, filt, load_sem.at[4])
    load(sinner_hbm, sinner, load_sem.at[1])

    def remote(source, target, send, recv, device):
        return pltpu.make_async_remote_copy(
            src_ref=source,
            dst_ref=target,
            send_sem=send,
            recv_sem=recv,
            device_id=device,
            device_id_type=MESH,
        )

    def to_next(buffer, c, send, recv):
        return remote(
            buffer.at[c, own], buffer.at[c, before], send.at[0], recv.at[c], seq(me + 1)
        )

    def to_relay(buffer, c, slot, send):
        return remote(
            buffer.at[c, own], relayed.at[slot], send.at[0], r_recv.at[slot], seq(me - 2)
        )

    k_copies = [to_next(keys, c, k_send, k_recv) for c in range(CHUNKS)]
    t_copies = [to_next(ext, c, t_send, t_recv) for c in range(CHUNKS)]
    v_copies = [to_next(values, c, v_send, v_recv) for c in range(CHUNKS)]
    lent_query = remote(
        query.at[:, last], next_query, lend_send.at[0], lend_recv.at[0], seq(me - 1)
    )
    lent_stats = remote(stats, stats_in, lend_send.at[1], lend_recv.at[1], seq(me + 1))
    lent_values = remote(
        lent, values.at[LENT, before], v_send.at[0], v_recv.at[LENT], seq(me + 1)
    )

    key_relay = [
        later > 1 if c >= HALF else True for c in range(CHUNKS)
    ]
    tail_relay = group == 0
    key_slot = [(c + HALF) % CHUNKS for c in range(CHUNKS)]

    def send_key(c, when=True):
        relay = jnp.logical_and(relays, key_relay[c])
        direct = jnp.logical_and(has_next, jnp.logical_not(relay))
        if c == LENT:
            direct = jnp.logical_and(direct, jnp.logical_not(lends))

        @pl.when(jnp.logical_and(relay, when))
        def _():
            to_relay(keys, c, key_slot[c], k_send).start()

        @pl.when(jnp.logical_and(direct, when))
        def _():
            k_copies[c].start()

    def send_tail(c):
        direct = has_next
        if c >= HALF:
            relay = jnp.logical_and(relays, tail_relay)
            direct = jnp.logical_and(has_next, jnp.logical_not(relay))

            @pl.when(relay)
            def _():
                to_relay(ext, c, CHUNKS + c - HALF, t_send).start()

        @pl.when(direct)
        def _():
            t_copies[c].start()

    def pass_on(buffer, c, slot, recv, when):
        @pl.when(jnp.logical_and(forwards, when))
        def _():
            remote(
                buffer.at[c, own], relayed.at[slot], k_send.at[0], r_recv.at[slot], seq(me + 2)
            ).wait_recv()
            remote(
                relayed.at[slot], buffer.at[c, before], r_send.at[0], recv.at[c], seq(me + 3)
            ).start()

    def pass_key(c):
        pass_on(keys, c, key_slot[c], k_recv, key_relay[c])

    def pass_tail(c):
        pass_on(ext, c, CHUNKS + c - HALF, t_recv, tail_relay)

    def pass_value():
        pass_on(values, 0, CHUNKS + HALF, v_recv, tail_relay)

    @pl.when(me == 0)
    def _():
        for c in range(CHUNKS):
            keys[c, :rows, :] = jnp.zeros((rows, wide), keys.dtype)
            values[c, :rows, :] = jnp.zeros((rows, wide), values.dtype)
            ext[c, :rows, :] = jnp.zeros((rows, wide), ext.dtype)

    pl.semaphore_wait(barrier, greeted)
    origin = group == 0
    late = jnp.logical_and(relays, origin)
    landed(query.at[:, last], load_sem.at[6])

    @pl.when(jnp.logical_and(borrows, jnp.logical_not(origin)))
    def _():
        lent_query.start()

    landed(keys.at[0, own], key_sem.at[0])
    send_key(0, jnp.logical_not(late))
    landed(keys.at[HALF, own], key_sem.at[1])
    for c in others:
        load_key(c, key_sem.at[2 + others.index(c)])
    load(souter_hbm, souter, load_sem.at[5])
    load(linner_hbm, linner, load_sem.at[5])
    load(louter_hbm, louter, load_sem.at[7])
    load(query_hbm.at[:, rest], query.at[:, rest], load_sem.at[8])
    landed(stream, load_sem.at[0])

    def square(i, acc):
        x = stream[:, pl.ds(pl.multiple_of(i * 128, 128), 128)].astype(jnp.float32)
        return acc + x * x

    total = lax.fori_loop(
        0, width // 128, square, jnp.zeros((rows, 128), jnp.float32), unroll=4
    )
    squares[...] = jnp.sum(total.T.reshape(128 // 8, 8, rows), axis=0)
    sq_copies = [
        pltpu.make_async_remote_copy(
            src_ref=squares,
            dst_ref=squares_in.at[k - 1],
            send_sem=sq_send.at[k - 1],
            recv_sem=sq_recv.at[k - 1],
            device_id={"mp": lax.rem(col + k, mp)},
            device_id_type=MESH,
        )
        for k in range(1, mp)
    ]
    for copy in sq_copies:
        copy.start()

    landed(vectors, load_sem.at[2])
    step = lax.broadcasted_iota(jnp.int32, (rows, TILE), 0).astype(jnp.float32)

    def powers(i, _):
        cols = pl.ds(pl.multiple_of(i * TILE, TILE), TILE)
        exponent = step * decay_ref[:, cols]
        power[:, cols] = jnp.exp(-exponent)
        inv_power[:, cols] = jnp.exp(exponent)
        return 0

    lax.fori_loop(0, width // TILE, powers, 0)
    landed(waves, load_sem.at[3])
    landed(filt, load_sem.at[4])

    def spectra(i, _):
        cols = pl.ds(pl.multiple_of(i * TILE, TILE), TILE)
        spectrum[:, cols] = dot(fwd[:, :rows], filt[:, cols])
        return 0

    lax.fori_loop(0, width // TILE // 2, spectra, 0)
    landed(sinner, load_sem.at[1])
    total = squares[...]
    for k, copy in enumerate(sq_copies):
        copy.wait_recv()
        total = total + squares_in[k]
    mean_square = jnp.sum(total, axis=0, keepdims=True) / channels
    norm = jnp.broadcast_to(1.0 / jnp.sqrt(mean_square + 0.5), (128, rows)).T
    norm = jnp.concatenate([norm] * (TILE // 128), axis=1)

    for c in range(CHUNKS):

        def short(i, _, c=c):
            cols = pl.ds(pl.multiple_of(c * wide + i * TILE, TILE), TILE)
            x = stream[:, cols].astype(jnp.float32) * gain_ref[:, cols] * norm
            ext[c, own, pl.ds(pl.multiple_of(i * TILE, TILE), TILE)] = (
                sinner[:, cols].astype(jnp.float32) * x
            ).astype(jnp.bfloat16)
            return 0

        lax.fori_loop(0, tiles, short, 0)
        send_tail(c)

    for i, c in enumerate(others):
        landed(keys.at[c, own], key_sem.at[2 + i])
    send_key(0, late)
    for c in range(1, CHUNKS):
        send_key(c)

    lax.fori_loop(width // TILE // 2, width // TILE, spectra, 0)
    landed(blocks.at[pl.ds(3, 2)], load_sem.at[5])
    row = lax.broadcasted_iota(jnp.int32, (rows, 2 * rows), 0)
    column = lax.broadcasted_iota(jnp.int32, (rows, 2 * rows), 1)
    lower = (jnp.where(column >= rows, column - rows, column) <= row).astype(
        jnp.float32
    ).astype(jnp.bfloat16)

    def state_copy(c, target, member):
        return remote(
            group_state.at[c],
            states.at[c, group],
            e_send.at[target],
            e_recv.at[c, group],
            seq(target * GROUP + member),
        )

    def mix_chunk(c):
        @pl.when(has_prev)
        def _():
            t_copies[c].wait_recv()

        def mix(i, _):
            here = pl.ds(pl.multiple_of(i * TILE, TILE), TILE)
            cols = pl.ds(pl.multiple_of(c * wide + i * TILE, TILE), TILE)
            x = dot(fwd[...], ext[c, :, here])
            x_re, x_im = x[:rows], x[rows:]
            h_re, h_im = spectrum[:rows, cols], spectrum[rows:, cols]
            y = jnp.concatenate(
                [x_re * h_re - x_im * h_im, x_re * h_im + x_im * h_re], axis=0
            ).astype(jnp.bfloat16)
            conv = dot(inv[...], y)
            long_in = (
                linner[:, cols].astype(jnp.float32) * souter[:, cols].astype(jnp.float32) * conv
            ).astype(jnp.bfloat16)
            v = long_in.astype(jnp.float32) * inv_power[:, cols]
            high = v.astype(jnp.bfloat16)
            low = (v - high.astype(jnp.float32)).astype(jnp.bfloat16)
            sums = dot(lower, jnp.concatenate([high, low], axis=0))
            cum[:, cols] = sums
            own_state[c, :, here] = sums[rows - 1 :] * power[rows - 1 :, cols]
            return 0

        lax.fori_loop(0, tiles, mix, 0)

        @pl.when(jnp.logical_not(even))
        def _():
            remote(
                own_state.at[c], member_state.at[c], p_send.at[0], p_recv.at[c], seq(me - 1)
            ).start()

    def rate_of(c):
        return decay_ref[:, pl.ds(c * wide, wide)]

    def pair(c):
        @pl.when(first)
        def _():
            landed(member_state.at[c], p_recv.at[c])
            over = jnp.exp(-rate_of(c) * rows)
            pair_state[c] = own_state[c] * over + member_state[c]
            remote(
                pair_state.at[c], before_state.at[c], g_send.at[0], g_recv.at[c], seq(me + 2)
            ).start()

    def collect(c):
        @pl.when(borrows)
        def _():
            landed(member_state.at[c], p_recv.at[c])
            landed(before_state.at[c], g_recv.at[c])
            over = jnp.exp(-rate_of(c) * rows)
            group_state[c] = (before_state[c] * over + own_state[c]) * over + member_state[c]

            def send_state(target, _):
                state_copy(c, target, 0).start()
                state_copy(c, target, 2).start()
                return 0

            lax.fori_loop(group + 1, groups, send_state, 0)

    def spread(c):
        @pl.when(even)
        def _():
            over_group = jnp.exp(-rate_of(c) * (rows * GROUP))

            def arrive(j, state):
                landed(states.at[c, j], e_recv.at[c, j])
                return state * over_group + states[c, j]

            state = lax.fori_loop(0, group, arrive, jnp.zeros((1, wide), jnp.float32))
            over = jnp.exp(-rate_of(c) * rows)
            carry_in[c] = state

            @pl.when(borrows)
            def _():
                carry_in[c] = state * jnp.exp(-rate_of(c) * (2 * rows)) + before_state[c]

            next_state[c] = carry_in[c] * over + own_state[c]
            remote(
                next_state.at[c], carry_in.at[c], q_send.at[0], q_recv.at[c], seq(me + 1)
            ).start()

    def long_chunk(c):
        @pl.when(jnp.logical_not(even))
        def _():
            landed(carry_in.at[c], q_recv.at[c])

        rate = rate_of(c)
        carried = carry_in[c] * jnp.exp(-rate)
        z = 2.0 * rate
        scale = jnp.sqrt(jnp.tanh(0.5 * z) * (1.0 + jnp.exp(-z)))
        for i in range(tiles):
            here = pl.ds(i * TILE, TILE)
            cols = pl.ds(c * wide + i * TILE, TILE)
            part = slice(i * TILE, (i + 1) * TILE)
            conv = (cum[:, cols] + carried[:, part]) * power[:, cols]
            out = (
                louter[:, cols].astype(jnp.float32) * (conv * scale[:, part])
            ).astype(jnp.bfloat16)
            values[c, own, here] = out
            mixed[:, cols] = out

        direct = has_next
        if c == LENT:
            direct = jnp.logical_and(has_next, jnp.logical_not(lends))

            @pl.when(lends)
            def _():
                def lend_values(h, _):
                    here = pl.ds(pl.multiple_of(h * HEAD_DIM, HEAD_DIM), HEAD_DIM)
                    lent[:, here] = dot_tn(
                        lent_weights[h], values[LENT, own, here]
                    ).astype(jnp.bfloat16)
                    return 0

                lax.fori_loop(0, heads, lend_values, 0, unroll=8)
                lent_values.start()

        if c == 0:
            relay = jnp.logical_and(relays, group == 0)
            direct = jnp.logical_and(has_next, jnp.logical_not(relay))

            @pl.when(relay)
            def _():
                to_relay(values, c, CHUNKS + HALF, v_send).start()

        if c < HALF:
            direct = jnp.logical_and(direct, jnp.logical_not(jnp.logical_and(relays, later > 1)))

        @pl.when(direct)
        def _():
            v_copies[c].start()

    def lend_weights():
        @pl.when(lends)
        def _():
            lent_query.wait_recv()
            for h in range(heads):
                here = pl.ds(h * HEAD_DIM, HEAD_DIM)
                s = dot_nt(keys[LENT, own, here], next_query[:, here]) * HEAD_DIM ** (-0.5)
                top = jnp.max(s, axis=0, keepdims=True)
                e = jnp.exp(s - top)
                total = jnp.sum(e, axis=0, keepdims=True)
                lent_weights[h] = (e * (1.0 / total)).astype(jnp.bfloat16)
                stats[h : h + 1, :] = top
                stats[heads + h : heads + h + 1, :] = total
            lent_stats.start()

    valid = (column <= row + rows) & ((column >= rows) | has_prev)

    def score_chunk(c, when=True):
        if c == LENT:
            when = jnp.logical_not(borrows)

        @pl.when(jnp.logical_and(has_prev, when))
        def _():
            k_copies[c].wait_recv()

        def score(h, _):
            here = pl.ds(pl.multiple_of(h * HEAD_DIM, HEAD_DIM), HEAD_DIM)
            cols = pl.ds(pl.multiple_of(c * wide + h * HEAD_DIM, HEAD_DIM), HEAD_DIM)
            s = dot_nt(query[:, cols], keys[c, :, here]) * HEAD_DIM ** (-0.5)
            s = jnp.where(valid, s, -1e30)
            e = jnp.exp(s - jnp.max(s, axis=1, keepdims=True))
            e = e * (1.0 / jnp.sum(e, axis=1, keepdims=True))
            weights[c, h] = e.astype(jnp.bfloat16)
            return 0

        def run():
            lax.fori_loop(0, heads, score, 0, unroll=2)

        if when is True:
            run()
        else:
            pl.when(when)(run)

    def borrow():
        @pl.when(borrows)
        def _():
            upper = lax.broadcasted_iota(
                jnp.int32, (rows, rows), 0
            ) <= lax.broadcasted_iota(jnp.int32, (rows, rows), 1)
            for h in range(heads):
                here = pl.ds(h * HEAD_DIM, HEAD_DIM)
                cols = pl.ds(LENT * wide + h * HEAD_DIM, HEAD_DIM)
                s = dot_nt(keys[LENT, own, here], query[:, cols]) * HEAD_DIM ** (-0.5)
                s = jnp.where(upper, s, -1e30)
                top = jnp.max(s, axis=0, keepdims=True)
                e = jnp.exp(s - top)
                lent_weights[h] = e.astype(jnp.bfloat16)
                stats[h : h + 1, :] = top
                stats[heads + h : heads + h + 1, :] = jnp.sum(e, axis=0, keepdims=True)
            for h in range(heads):
                here = pl.ds(h * HEAD_DIM, HEAD_DIM)
                own_part[:, here] = dot_tn(lent_weights[h], values[LENT, own, here])

    def blend():
        @pl.when(borrows)
        def _():
            lent_stats.wait_recv()
            top, total = stats[:heads], stats[heads:]
            top_before, total_before = stats_in[:heads], stats_in[heads:]
            most = jnp.maximum(top, top_before)
            here_scale = jnp.exp(top - most)
            before_scale = jnp.exp(top_before - most) * total_before
            inverse = 1.0 / (total * here_scale + before_scale)
            both = jnp.concatenate([here_scale * inverse, before_scale * inverse], axis=0)
            both = jnp.concatenate(
                [both, jnp.zeros((HEAD_DIM - 2 * heads, rows), jnp.float32)], axis=0
            ).T
            for h in range(heads):
                here = pl.ds(h * HEAD_DIM, HEAD_DIM)
                own_part[:, here] = own_part[:, here] * both[:, h : h + 1]
                shares[:, here] = jnp.broadcast_to(
                    both[:, heads + h : heads + h + 1], (rows, HEAD_DIM)
                )

    def attend_chunk(c):
        @pl.when(has_prev)
        def _():
            v_copies[c].wait_recv()

        def gather(h, _):
            here = pl.ds(pl.multiple_of(h * HEAD_DIM, HEAD_DIM), HEAD_DIM)
            cols = pl.ds(pl.multiple_of(c * wide + h * HEAD_DIM, HEAD_DIM), HEAD_DIM)
            attended[:, cols] = dot(weights[c, h], values[c, :, here]).astype(jnp.bfloat16)
            return 0

        def finish():
            lax.fori_loop(0, heads, gather, 0, unroll=8)

        if c < LENT:
            finish()
            return
        pl.when(jnp.logical_not(borrows))(finish)

        @pl.when(borrows)
        def _():
            for i in range(tiles):
                here = pl.ds(i * TILE, TILE)
                cols = pl.ds(c * wide + i * TILE, TILE)
                attended[:, cols] = (
                    own_part[:, here]
                    + shares[:, here] * values[c, before, here].astype(jnp.float32)
                ).astype(jnp.bfloat16)

    mix_chunk(0)
    pair(0)
    pass_tail(2)
    mix_chunk(1)
    pair(1)
    collect(0)

    @pl.when(jnp.logical_and(borrows, origin))
    def _():
        lent_query.start()

    pass_tail(3)
    mix_chunk(2)
    pair(2)
    collect(1)
    landed(louter, load_sem.at[7])
    landed(query.at[:, rest], load_sem.at[8])
    spread(0)
    mix_chunk(3)
    pair(3)
    collect(2)
    spread(1)
    pass_key(0)
    long_chunk(0)
    long_chunk(1)
    pass_key(1)
    pass_key(2)
    score_chunk(0, jnp.logical_not(first))

    @pl.when(relays & (group > 0) & (later > 1))
    def _():
        v_copies[0].start()

    for c in range(1, HALF):

        @pl.when(jnp.logical_and(relays, later > 1))
        def _(c=c):
            v_copies[c].start()

    collect(3)
    spread(2)
    long_chunk(2)
    lend_weights()
    pass_key(3)
    score_chunk(1, jnp.logical_not(first))
    spread(3)
    long_chunk(3)
    pass_value()
    score_chunk(0, first)
    score_chunk(1, first)
    score_chunk(2)
    score_chunk(3)
    borrow()
    for c in range(CHUNKS - 1):
        attend_chunk(c)
    blend()
    attend_chunk(LENT)

    for copy in sq_copies:
        copy.wait_send()

    def sent(buffer, sem):
        pltpu.make_async_copy(buffer, buffer, sem).wait()

    @pl.when(jnp.logical_not(even))
    def _():
        sent(own_state, p_send.at[0])

    @pl.when(even)
    def _():
        sent(next_state, q_send.at[0])

    @pl.when(first)
    def _():
        sent(pair_state, g_send.at[0])

    @pl.when(borrows)
    def _():
        lent_query.wait_send()

        def all_sent(target, _):
            sent(states.at[:, pl.ds(0, 2)], e_send.at[target])
            return 0

        lax.fori_loop(group + 1, groups, all_sent, 0)

    for tails in (True, False):
        for fewer in (True, False):
            slots = pl.ds(HALF if fewer else 0, CHUNKS + tails * (HALF + 1) - fewer * HALF)

            @pl.when(forwards & (tail_relay == tails) & ((later == 1) == fewer))
            def _(slots=slots):
                sent(relayed.at[slots], r_send.at[0])

    @pl.when(lends)
    def _():
        sent(keys.at[pl.ds(0, LENT), own], k_send.at[0])
        lent_stats.wait_send()

    @pl.when(jnp.logical_and(has_next, jnp.logical_not(lends)))
    def _():
        sent(keys.at[:, own], k_send.at[0])

    @pl.when(has_next)
    def _():
        sent(ext.at[:, own], t_send.at[0])
        sent(values.at[:, own], v_send.at[0])


def store(mixed, attended, mixed_hbm, attended_hbm, sem):
    rows = mixed.shape[0]
    parts = [pl.ds(i * rows // STORES, rows // STORES) for i in range(STORES)]
    copies = [
        pltpu.make_async_copy(source.at[part], target.at[part], sem.at[k, i])
        for k, (source, target) in enumerate([(mixed, mixed_hbm), (attended, attended_hbm)])
        for i, part in enumerate(parts)
    ]
    for copy in copies:
        copy.start()
    for copy in copies:
        copy.wait()


def on_device(
    n,
    mp,
    stream,
    norm_gain,
    short_outer,
    short_inner,
    short_filter,
    long_outer,
    long_inner,
    long_decay,
    query_heads,
    key_heads,
):
    rows, width = stream.shape
    wide = width // CHUNKS
    heads = wide // HEAD_DIM
    groups = n // GROUP
    bf16, f32 = jnp.bfloat16, jnp.float32
    anywhere = pl.BlockSpec(memory_space=pltpu.HBM)
    vmem = pl.BlockSpec(memory_space=pltpu.VMEM)
    dma = pltpu.SemaphoreType.DMA

    def in_hbm(array):
        return pltpu.with_memory_space_constraint(array, pltpu.HBM)

    mixed, attended = pl.pallas_call(
        functools.partial(kernel, n, mp, float(width * mp)),
        out_shape=[jax.ShapeDtypeStruct((rows, width), bf16)] * 2,
        in_specs=[anywhere] * 11,
        out_specs=[vmem] * 2,
        scratch_shapes=[
            pltpu.VMEM((2, 1, width), f32),
            pltpu.VMEM((7, rows, width), bf16),
            pltpu.VMEM((3 * rows, 2 * rows), bf16),
        ]
        + [pltpu.VMEM((CHUNKS, 2 * rows, wide), bf16)] * 3
        + [pltpu.VMEM((CHUNKS + HALF + 1, rows, wide), bf16)]
        + [pltpu.VMEM((rows, wide), bf16)] * 2
        + [pltpu.VMEM((rows, wide), f32)] * 2
        + [pltpu.VMEM((rows, width), f32)] * 3
        + [
            pltpu.VMEM((2 * rows, width), f32),
            pltpu.VMEM((CHUNKS, heads, rows, 2 * rows), bf16),
            pltpu.VMEM((heads, rows, rows), bf16),
        ]
        + [pltpu.VMEM((2 * heads, rows), f32)] * 2
        + [
            pltpu.VMEM((8, rows), f32),
            pltpu.VMEM((mp - 1, 8, rows), f32),
        ]
        + [pltpu.VMEM((CHUNKS, 1, wide), f32)] * 7
        + [
            pltpu.VMEM((CHUNKS, groups, 1, wide), f32),
            dma((9,)),
            dma((CHUNKS,)),
            dma((mp - 1,)),
            dma((mp - 1,)),
        ]
        + [dma((1,)), dma((CHUNKS,))] * 3
        + [dma((1,)), dma((CHUNKS + HALF + 1,))]
        + [dma((1,)), dma((CHUNKS,))] * 3
        + [dma((groups,)), dma((CHUNKS, groups))]
        + [dma((2,))] * 2,
        compiler_params=pltpu.CompilerParams(
            collective_id=0, has_side_effects=True, vmem_limit_bytes=51 * 1024 * 1024
        ),
    )(
        in_hbm(norm_gain.reshape(1, width)),
        in_hbm(long_decay.reshape(1, width)),
        in_hbm(jnp.asarray(waves_of(rows), bf16)),
        stream,
        short_outer,
        short_inner,
        short_filter,
        long_outer,
        long_inner,
        query_heads,
        key_heads,
    )
    return pl.pallas_call(
        store,
        out_shape=[jax.ShapeDtypeStruct((rows, width), bf16)] * 2,
        in_specs=[vmem] * 2,
        out_specs=[anywhere] * 2,
        scratch_shapes=[dma((2, STORES))],
        compiler_params=pltpu.CompilerParams(vmem_limit_bytes=1024 * 1024),
    )(mixed, attended)


def solution(mesh):
    return jax.shard_map(
        functools.partial(on_device, mesh.shape["seq"], mesh.shape["mp"]),
        mesh=mesh,
        in_specs=(
            P("seq", "mp"),
            P("mp"),
            P("seq", "mp"),
            P("seq", "mp"),
            P(None, "mp"),
            P("seq", "mp"),
            P("seq", "mp"),
            P("mp"),
            P("seq", "mp"),
            P("seq", "mp"),
        ),
        out_specs=(P("seq", "mp"), P("seq", "mp")),
        check_vma=False,
    )
```

```python
import functools

import jax
import jax.numpy as jnp
import numpy as np
from jax import lax
from jax.experimental import pallas as pl
from jax.experimental.pallas import tpu as pltpu
from jax.sharding import PartitionSpec as P

HEAD_DIM = 128
CHUNKS = 4
HALF = CHUNKS // 2
LENT = CHUNKS - 1
GROUP = 4
TILE = 256
STORES = 2
MESH = pl.DeviceIdType.MESH


def wave(frequency, place, rows):
    shift = np.where(frequency >= rows, rows, 0)
    index = ((2 * (frequency % rows) + 1) * place + shift) % (4 * rows)
    return np.cos(index * (np.pi / (2 * rows)))


def waves_of(rows):
    every = np.arange(2 * rows)
    fwd = wave(every[:, None], every[None, :], rows)
    inv = wave(every[None, :], every[:rows, None] + rows, rows) / rows
    return np.concatenate([fwd, inv], axis=0)


def dot(a, b):
    return jnp.dot(a, b, preferred_element_type=jnp.float32)


def dot_nt(a, b):
    return lax.dot_general(a, b, (((1,), (1,)), ((), ())), preferred_element_type=jnp.float32)


def dot_tn(a, b):
    return lax.dot_general(a, b, (((0,), (0,)), ((), ())), preferred_element_type=jnp.float32)


def kernel(
    n,
    mp,
    channels,
    gain_hbm,
    decay_hbm,
    waves_hbm,
    stream_hbm,
    souter_hbm,
    sinner_hbm,
    filt_hbm,
    louter_hbm,
    linner_hbm,
    query_hbm,
    key_hbm,
    mixed,
    attended,
    vectors,
    blocks,
    waves,
    keys,
    values,
    ext,
    relayed,
    next_query,
    lent,
    own_part,
    shares,
    power,
    inv_power,
    cum,
    spectrum,
    weights,
    lent_weights,
    stats,
    stats_in,
    squares,
    squares_in,
    own_state,
    member_state,
    pair_state,
    before_state,
    group_state,
    next_state,
    across_state,
    carry_in,
    states,
    load_sem,
    key_sem,
    sq_send,
    sq_recv,
    k_send,
    k_recv,
    t_send,
    t_recv,
    v_send,
    v_recv,
    cross_send,
    cross_recv,
    state_send,
    state_recv,
    e_send,
    e_recv,
    lend_send,
    lend_recv,
):
    gain_ref, decay_ref = vectors.at[0], vectors.at[1]
    stream, sinner, filt, souter, linner, louter, query = (blocks.at[i] for i in range(7))
    me = lax.axis_index("seq")
    col = lax.axis_index("mp")
    rows, width = stream.shape
    fwd, inv = waves.at[pl.ds(0, 2 * rows)], waves.at[pl.ds(2 * rows, rows)]
    wide = width // CHUNKS
    tiles = wide // TILE
    heads = wide // HEAD_DIM
    has_next = me < n - 1
    has_prev = me > 0
    groups = n // GROUP
    group = me // GROUP
    role = lax.rem(me, GROUP)
    later = groups - 1 - group
    first = role == 0
    lends = role == 1
    borrows = role == 2
    relays = jnp.logical_and(role == 3, later > 0)
    forwards = jnp.logical_and(lends, later > 0)
    even = lax.rem(me, 2) == 0
    own = pl.ds(rows, rows)
    before = pl.ds(0, rows)

    def seq(target):
        return {"seq": lax.rem(target + n, n)}

    barrier = pltpu.get_barrier_semaphore()

    def greet(target, when):
        @pl.when(when)
        def _():
            pl.semaphore_signal(barrier, inc=1, device_id=seq(target), device_id_type=MESH)

    greet(me + 1, has_next)
    greet(me - 1, has_prev)
    greet(me - 2, borrows)
    greet(me + 2, forwards)
    greet(me - 3, jnp.logical_and(first, group > 0))

    @pl.when(first)
    def _():
        def greet_earlier(j, _):
            pl.semaphore_signal(
                barrier, inc=1, device_id=seq(j * GROUP + 2), device_id_type=MESH
            )
            return 0

        lax.fori_loop(0, group, greet_earlier, 0)

    greeted = has_next.astype(jnp.int32) + has_prev.astype(jnp.int32) + mp - 1
    greeted += jnp.where(borrows, later, 0)
    greeted += (first | relays | forwards).astype(jnp.int32)

    for k in range(1, mp):
        pl.semaphore_signal(
            barrier, inc=1, device_id={"mp": lax.rem(col + k, mp)}, device_id_type=MESH
        )

    def load(source, target, sem):
        pltpu.make_async_copy(source, target, sem).start()

    def landed(buffer, sem):
        pltpu.make_async_copy(buffer, buffer, sem).wait()

    def load_key(c, sem):
        load(key_hbm.at[:, pl.ds(c * wide, wide)], keys.at[c, own], sem)

    last = pl.ds(LENT * wide, wide)
    rest = pl.ds(0, LENT * wide)
    load(query_hbm.at[:, last], query.at[:, last], load_sem.at[6])
    load_key(0, key_sem.at[0])
    load_key(HALF, key_sem.at[1])
    load(stream_hbm, stream, load_sem.at[0])
    load(gain_hbm, gain_ref, load_sem.at[2])
    load(decay_hbm, decay_ref, load_sem.at[2])

    def remote(source, target, send, recv, device):
        return pltpu.make_async_remote_copy(
            src_ref=source,
            dst_ref=target,
            send_sem=send,
            recv_sem=recv,
            device_id=device,
            device_id_type=MESH,
        )

    def to_next(buffer, c, send, recv):
        return remote(
            buffer.at[c, own], buffer.at[c, before], send.at[0], recv.at[c], seq(me + 1)
        )

    def to_relay(buffer, c, slot, send):
        return remote(
            buffer.at[c, own], relayed.at[slot], send.at[0], cross_recv.at[slot], seq(me - 2)
        )

    k_copies = [to_next(keys, c, k_send, k_recv) for c in range(CHUNKS)]
    t_copies = [to_next(ext, c, t_send, t_recv) for c in range(CHUNKS)]
    v_copies = [to_next(values, c, v_send, v_recv) for c in range(CHUNKS)]
    lent_query = remote(
        query.at[:, last], next_query, lend_send.at[0], lend_recv.at[0], seq(me - 1)
    )
    lent_stats = remote(stats, stats_in, lend_send.at[1], lend_recv.at[1], seq(me + 1))
    lent_values = remote(
        lent, values.at[LENT, before], v_send.at[0], v_recv.at[LENT], seq(me + 1)
    )

    key_relay = [
        later > 1 if c >= HALF else True for c in range(CHUNKS)
    ]
    tail_relay = group == 0
    key_slot = [(c + HALF) % CHUNKS for c in range(CHUNKS)]

    def send_key(c, when=True):
        relay = jnp.logical_and(relays, key_relay[c])
        direct = jnp.logical_and(has_next, jnp.logical_not(relay))
        if c == LENT:
            direct = jnp.logical_and(direct, jnp.logical_not(lends))

        @pl.when(jnp.logical_and(relay, when))
        def _():
            to_relay(keys, c, key_slot[c], k_send).start()

        @pl.when(jnp.logical_and(direct, when))
        def _():
            k_copies[c].start()

    def send_tail(c):
        direct = has_next
        if c >= HALF:
            relay = jnp.logical_and(relays, tail_relay)
            direct = jnp.logical_and(has_next, jnp.logical_not(relay))

            @pl.when(relay)
            def _():
                to_relay(ext, c, CHUNKS + c - HALF, t_send).start()

        @pl.when(direct)
        def _():
            t_copies[c].start()

    def pass_on(buffer, c, slot, recv, when):
        @pl.when(jnp.logical_and(forwards, when))
        def _():
            remote(
                buffer.at[c, own], relayed.at[slot], k_send.at[0], cross_recv.at[slot], seq(me + 2)
            ).wait_recv()
            remote(
                relayed.at[slot], buffer.at[c, before], cross_send.at[0], recv.at[c], seq(me + 3)
            ).start()

    def pass_key(c):
        pass_on(keys, c, key_slot[c], k_recv, key_relay[c])

    def pass_tail(c):
        pass_on(ext, c, CHUNKS + c - HALF, t_recv, tail_relay)

    def pass_value():
        pass_on(values, 0, CHUNKS + HALF, v_recv, tail_relay)

    @pl.when(me == 0)
    def _():
        for c in range(CHUNKS):
            keys[c, :rows, :] = jnp.zeros((rows, wide), keys.dtype)
            values[c, :rows, :] = jnp.zeros((rows, wide), values.dtype)
            ext[c, :rows, :] = jnp.zeros((rows, wide), ext.dtype)

    pl.semaphore_wait(barrier, greeted)
    origin = group == 0
    late = jnp.logical_and(relays, origin)
    landed(query.at[:, last], load_sem.at[6])

    @pl.when(jnp.logical_and(borrows, jnp.logical_not(origin)))
    def _():
        lent_query.start()

    landed(keys.at[0, own], key_sem.at[0])
    send_key(0, jnp.logical_not(late))
    ahead = jnp.logical_and(relays, later == 1)
    landed(keys.at[HALF, own], key_sem.at[1])
    send_key(HALF, ahead)
    load(waves_hbm, waves, load_sem.at[3])
    load(filt_hbm, filt, load_sem.at[4])
    load(sinner_hbm, sinner, load_sem.at[1])
    others = [c for c in range(1, CHUNKS) if c != HALF]
    for i, c in enumerate(others):
        load_key(c, key_sem.at[2 + i])
    load(souter_hbm, souter, load_sem.at[5])
    load(linner_hbm, linner, load_sem.at[5])
    load(louter_hbm, louter, load_sem.at[5])
    load(query_hbm.at[:, rest], query.at[:, rest], load_sem.at[7])
    landed(stream, load_sem.at[0])

    def square(i, acc):
        x = stream[:, pl.ds(pl.multiple_of(i * 128, 128), 128)].astype(jnp.float32)
        return acc + x * x

    total = lax.fori_loop(
        0, width // 128, square, jnp.zeros((rows, 128), jnp.float32), unroll=4
    )
    squares[...] = jnp.sum(total.T.reshape(128 // 8, 8, rows), axis=0)
    sq_copies = [
        pltpu.make_async_remote_copy(
            src_ref=squares,
            dst_ref=squares_in.at[k - 1],
            send_sem=sq_send.at[k - 1],
            recv_sem=sq_recv.at[k - 1],
            device_id={"mp": lax.rem(col + k, mp)},
            device_id_type=MESH,
        )
        for k in range(1, mp)
    ]
    for copy in sq_copies:
        copy.start()

    landed(vectors, load_sem.at[2])
    step = lax.broadcasted_iota(jnp.int32, (rows, TILE), 0).astype(jnp.float32)

    def powers(i, _):
        cols = pl.ds(pl.multiple_of(i * TILE, TILE), TILE)
        exponent = step * decay_ref[:, cols]
        power[:, cols] = jnp.exp(-exponent)
        inv_power[:, cols] = jnp.exp(exponent)
        return 0

    lax.fori_loop(0, width // TILE, powers, 0)
    landed(waves, load_sem.at[3])
    landed(filt, load_sem.at[4])

    def spectra(i, _):
        cols = pl.ds(pl.multiple_of(i * TILE, TILE), TILE)
        spectrum[:, cols] = dot(fwd[:, :rows], filt[:, cols])
        return 0

    lax.fori_loop(0, width // TILE // 2, spectra, 0)
    landed(sinner, load_sem.at[1])
    total = squares[...]
    for k, copy in enumerate(sq_copies):
        copy.wait_recv()
        total = total + squares_in[k]
    mean_square = jnp.sum(total, axis=0, keepdims=True) / channels
    norm = jnp.broadcast_to(1.0 / jnp.sqrt(mean_square + 0.5), (128, rows)).T
    norm = jnp.concatenate([norm] * (TILE // 128), axis=1)

    for c in range(CHUNKS):

        def short(i, _, c=c):
            cols = pl.ds(pl.multiple_of(c * wide + i * TILE, TILE), TILE)
            x = stream[:, cols].astype(jnp.float32) * gain_ref[:, cols] * norm
            ext[c, own, pl.ds(pl.multiple_of(i * TILE, TILE), TILE)] = (
                sinner[:, cols].astype(jnp.float32) * x
            ).astype(jnp.bfloat16)
            return 0

        lax.fori_loop(0, tiles, short, 0)
        send_tail(c)

    for i, c in enumerate(others):
        landed(keys.at[c, own], key_sem.at[2 + i])
    send_key(0, late)
    for c in range(1, CHUNKS):
        send_key(c, jnp.logical_not(ahead) if c == HALF else True)

    lax.fori_loop(width // TILE // 2, width // TILE, spectra, 0)
    landed(blocks.at[pl.ds(3, 3)], load_sem.at[5])
    row = lax.broadcasted_iota(jnp.int32, (rows, 2 * rows), 0)
    column = lax.broadcasted_iota(jnp.int32, (rows, 2 * rows), 1)
    lower = (jnp.where(column >= rows, column - rows, column) <= row).astype(
        jnp.float32
    ).astype(jnp.bfloat16)

    def state_copy(c, target):
        return remote(
            group_state.at[c],
            states.at[c, group],
            e_send.at[target],
            e_recv.at[c],
            seq(target * GROUP),
        )

    def mix_chunk(c):
        @pl.when(has_prev)
        def _():
            t_copies[c].wait_recv()

        def mix(i, _):
            here = pl.ds(pl.multiple_of(i * TILE, TILE), TILE)
            cols = pl.ds(pl.multiple_of(c * wide + i * TILE, TILE), TILE)
            x = dot(fwd[...], ext[c, :, here])
            x_re, x_im = x[:rows], x[rows:]
            h_re, h_im = spectrum[:rows, cols], spectrum[rows:, cols]
            y = jnp.concatenate(
                [x_re * h_re - x_im * h_im, x_re * h_im + x_im * h_re], axis=0
            ).astype(jnp.bfloat16)
            conv = dot(inv[...], y)
            long_in = (
                linner[:, cols].astype(jnp.float32) * souter[:, cols].astype(jnp.float32) * conv
            ).astype(jnp.bfloat16)
            v = long_in.astype(jnp.float32) * inv_power[:, cols]
            high = v.astype(jnp.bfloat16)
            low = (v - high.astype(jnp.float32)).astype(jnp.bfloat16)
            sums = dot(lower, jnp.concatenate([high, low], axis=0))
            cum[:, cols] = sums
            own_state[c, :, here] = sums[rows - 1 :] * power[rows - 1 :, cols]
            return 0

        lax.fori_loop(0, tiles, mix, 0)

        @pl.when(jnp.logical_not(even))
        def _():
            remote(
                own_state.at[c], member_state.at[c], state_send.at[0], state_recv.at[c], seq(me - 1)
            ).start()

    def rate_of(c):
        return decay_ref[:, pl.ds(c * wide, wide)]

    def pair(c):
        @pl.when(first)
        def _():
            landed(member_state.at[c], state_recv.at[c])
            over = jnp.exp(-rate_of(c) * rows)
            pair_state[c] = own_state[c] * over + member_state[c]
            remote(
                pair_state.at[c], before_state.at[c], cross_send.at[0], cross_recv.at[c], seq(me + 2)
            ).start()

    def collect(c):
        @pl.when(borrows)
        def _():
            landed(member_state.at[c], state_recv.at[c])
            landed(before_state.at[c], cross_recv.at[c])
            over = jnp.exp(-rate_of(c) * rows)
            group_state[c] = (before_state[c] * over + own_state[c]) * over + member_state[c]

            def send_state(target, _):
                state_copy(c, target).start()
                return 0

            lax.fori_loop(group + 1, groups, send_state, 0)

    def spread(c):
        @pl.when(first)
        def _():
            for g in range(1, groups):

                @pl.when(group == g)
                def _(g=g):
                    landed(states.at[c, pl.ds(0, g)], e_recv.at[c])

            over_group = jnp.exp(-rate_of(c) * (rows * GROUP))

            def arrive(j, state):
                return state * over_group + states[c, j]

            state = lax.fori_loop(0, group, arrive, jnp.zeros((1, wide), jnp.float32))
            over = jnp.exp(-rate_of(c) * rows)
            carry_in[c] = state
            next_state[c] = state * over + own_state[c]
            give_next(c)
            across_state[c] = state * jnp.exp(-rate_of(c) * (2 * rows)) + pair_state[c]
            remote(
                across_state.at[c], carry_in.at[c], cross_send.at[1], e_recv.at[c], seq(me + 2)
            ).start()

    def give_next(c):
        remote(
            next_state.at[c], carry_in.at[c], state_send.at[0], state_recv.at[c], seq(me + 1)
        ).start()

    def hand_on(c):
        @pl.when(borrows)
        def _():
            landed(carry_in.at[c], e_recv.at[c])
            next_state[c] = carry_in[c] * jnp.exp(-rate_of(c) * rows) + own_state[c]
            give_next(c)

    def long_chunk(c):
        @pl.when(jnp.logical_not(even))
        def _():
            landed(carry_in.at[c], state_recv.at[c])

        rate = rate_of(c)
        carried = carry_in[c] * jnp.exp(-rate)
        z = 2.0 * rate
        scale = jnp.sqrt(jnp.tanh(0.5 * z) * (1.0 + jnp.exp(-z)))
        for i in range(tiles):
            here = pl.ds(i * TILE, TILE)
            cols = pl.ds(c * wide + i * TILE, TILE)
            part = slice(i * TILE, (i + 1) * TILE)
            conv = (cum[:, cols] + carried[:, part]) * power[:, cols]
            out = (
                louter[:, cols].astype(jnp.float32) * (conv * scale[:, part])
            ).astype(jnp.bfloat16)
            values[c, own, here] = out
            mixed[:, cols] = out

        direct = has_next
        if c == LENT:
            direct = jnp.logical_and(has_next, jnp.logical_not(lends))

            @pl.when(lends)
            def _():
                def lend_values(h, _):
                    here = pl.ds(pl.multiple_of(h * HEAD_DIM, HEAD_DIM), HEAD_DIM)
                    lent[:, here] = dot_tn(
                        lent_weights[h], values[LENT, own, here]
                    ).astype(jnp.bfloat16)
                    return 0

                lax.fori_loop(0, heads, lend_values, 0, unroll=8)
                lent_values.start()

        if c == 0:
            relay = jnp.logical_and(relays, group == 0)
            direct = jnp.logical_and(has_next, jnp.logical_not(relay))

            @pl.when(relay)
            def _():
                to_relay(values, c, CHUNKS + HALF, v_send).start()

        if c == 0:
            direct = jnp.logical_and(direct, jnp.logical_not(held))

        @pl.when(direct)
        def _():
            v_copies[c].start()

    def lend_weights():
        @pl.when(lends)
        def _():
            lent_query.wait_recv()
            for h in range(heads):
                here = pl.ds(h * HEAD_DIM, HEAD_DIM)
                s = dot_nt(keys[LENT, own, here], next_query[:, here]) * HEAD_DIM ** (-0.5)
                top = jnp.max(s, axis=0, keepdims=True)
                e = jnp.exp(s - top)
                total = jnp.sum(e, axis=0, keepdims=True)
                lent_weights[h] = (e * (1.0 / total)).astype(jnp.bfloat16)
                stats[h : h + 1, :] = top
                stats[heads + h : heads + h + 1, :] = total
            lent_stats.start()

    valid = (column <= row + rows) & ((column >= rows) | has_prev)

    def score_chunk(c, when=True, half=None):
        if c == LENT:
            when = jnp.logical_not(borrows)

        @pl.when(jnp.logical_and(has_prev, when if half != 1 else False))
        def _():
            k_copies[c].wait_recv()

        def score(h, _):
            here = pl.ds(pl.multiple_of(h * HEAD_DIM, HEAD_DIM), HEAD_DIM)
            cols = pl.ds(pl.multiple_of(c * wide + h * HEAD_DIM, HEAD_DIM), HEAD_DIM)
            s = dot_nt(query[:, cols], keys[c, :, here]) * HEAD_DIM ** (-0.5)
            s = jnp.where(valid, s, -1e30)
            e = jnp.exp(s - jnp.max(s, axis=1, keepdims=True))
            e = e * (1.0 / jnp.sum(e, axis=1, keepdims=True))
            weights[c, h] = e.astype(jnp.bfloat16)
            return 0

        start = heads // 2 if half == 1 else 0
        stop = heads // 2 if half == 0 else heads

        def run():
            lax.fori_loop(start, stop, score, 0, unroll=2)

        if when is True:
            run()
        else:
            pl.when(when)(run)

    def borrow():
        @pl.when(borrows)
        def _():
            upper = lax.broadcasted_iota(
                jnp.int32, (rows, rows), 0
            ) <= lax.broadcasted_iota(jnp.int32, (rows, rows), 1)
            for h in range(heads):
                here = pl.ds(h * HEAD_DIM, HEAD_DIM)
                cols = pl.ds(LENT * wide + h * HEAD_DIM, HEAD_DIM)
                s = dot_nt(keys[LENT, own, here], query[:, cols]) * HEAD_DIM ** (-0.5)
                s = jnp.where(upper, s, -1e30)
                top = jnp.max(s, axis=0, keepdims=True)
                e = jnp.exp(s - top)
                lent_weights[h] = e.astype(jnp.bfloat16)
                stats[h : h + 1, :] = top
                stats[heads + h : heads + h + 1, :] = jnp.sum(e, axis=0, keepdims=True)
            for h in range(heads):
                here = pl.ds(h * HEAD_DIM, HEAD_DIM)
                own_part[:, here] = dot_tn(lent_weights[h], values[LENT, own, here])

    def blend():
        @pl.when(borrows)
        def _():
            lent_stats.wait_recv()
            top, total = stats[:heads], stats[heads:]
            top_before, total_before = stats_in[:heads], stats_in[heads:]
            most = jnp.maximum(top, top_before)
            here_scale = jnp.exp(top - most)
            before_scale = jnp.exp(top_before - most) * total_before
            inverse = 1.0 / (total * here_scale + before_scale)
            both = jnp.concatenate([here_scale * inverse, before_scale * inverse], axis=0)
            both = jnp.concatenate(
                [both, jnp.zeros((HEAD_DIM - 2 * heads, rows), jnp.float32)], axis=0
            ).T
            for h in range(heads):
                here = pl.ds(h * HEAD_DIM, HEAD_DIM)
                own_part[:, here] = own_part[:, here] * both[:, h : h + 1]
                shares[:, here] = jnp.broadcast_to(
                    both[:, heads + h : heads + h + 1], (rows, HEAD_DIM)
                )

    def attend_chunk(c):
        @pl.when(has_prev)
        def _():
            v_copies[c].wait_recv()

        def gather(h, _):
            here = pl.ds(pl.multiple_of(h * HEAD_DIM, HEAD_DIM), HEAD_DIM)
            cols = pl.ds(pl.multiple_of(c * wide + h * HEAD_DIM, HEAD_DIM), HEAD_DIM)
            attended[:, cols] = dot(weights[c, h], values[c, :, here]).astype(jnp.bfloat16)
            return 0

        def finish():
            lax.fori_loop(0, heads, gather, 0, unroll=8)

        if c < LENT:
            finish()
            return
        pl.when(jnp.logical_not(borrows))(finish)

        @pl.when(borrows)
        def _():
            for i in range(tiles):
                here = pl.ds(i * TILE, TILE)
                cols = pl.ds(c * wide + i * TILE, TILE)
                attended[:, cols] = (
                    own_part[:, here]
                    + shares[:, here] * values[c, before, here].astype(jnp.float32)
                ).astype(jnp.bfloat16)

    mix_chunk(0)
    pair(0)
    pass_tail(2)
    mix_chunk(1)
    pair(1)
    collect(0)

    @pl.when(jnp.logical_and(borrows, origin))
    def _():
        lent_query.start()

    pass_tail(3)
    mix_chunk(2)
    pair(2)
    collect(1)
    landed(query.at[:, rest], load_sem.at[7])
    spread(0)
    mix_chunk(3)
    pair(3)
    collect(2)
    spread(1)
    pass_key(0)
    hand_on(0)
    held = relays & (group > 0)
    long_chunk(0)
    score_chunk(0, jnp.logical_not(first), 0)

    @pl.when(held)
    def _():
        v_copies[0].start()

    score_chunk(0, jnp.logical_not(first), 1)
    collect(3)
    spread(2)
    hand_on(1)
    long_chunk(1)
    pass_key(1)
    pass_key(2)
    hand_on(2)
    long_chunk(2)
    lend_weights()
    pass_key(3)
    score_chunk(1, jnp.logical_not(first))
    spread(3)
    hand_on(3)
    long_chunk(3)
    pass_value()
    score_chunk(0, first)
    score_chunk(1, first)
    score_chunk(2)
    score_chunk(3)
    borrow()
    for c in range(CHUNKS - 1):
        attend_chunk(c)
    blend()
    attend_chunk(LENT)

    for copy in sq_copies:
        copy.wait_send()

    def sent(buffer, sem):
        pltpu.make_async_copy(buffer, buffer, sem).wait()

    @pl.when(jnp.logical_not(even))
    def _():
        sent(own_state, state_send.at[0])

    @pl.when(even)
    def _():
        sent(next_state, state_send.at[0])

    @pl.when(first)
    def _():
        sent(pair_state, cross_send.at[0])
        sent(across_state, cross_send.at[1])

    @pl.when(borrows)
    def _():
        lent_query.wait_send()

        def all_sent(target, _):
            sent(group_state, e_send.at[target])
            return 0

        lax.fori_loop(group + 1, groups, all_sent, 0)

    for tails in (True, False):
        for fewer in (True, False):
            slots = pl.ds(HALF if fewer else 0, CHUNKS + tails * (HALF + 1) - fewer * HALF)

            @pl.when(forwards & (tail_relay == tails) & ((later == 1) == fewer))
            def _(slots=slots):
                sent(relayed.at[slots], cross_send.at[0])

    @pl.when(lends)
    def _():
        sent(keys.at[pl.ds(0, LENT), own], k_send.at[0])
        lent_stats.wait_send()

    @pl.when(jnp.logical_and(has_next, jnp.logical_not(lends)))
    def _():
        sent(keys.at[:, own], k_send.at[0])

    @pl.when(has_next)
    def _():
        sent(ext.at[:, own], t_send.at[0])
        sent(values.at[:, own], v_send.at[0])


def store(mixed, attended, mixed_hbm, attended_hbm, sem):
    rows = mixed.shape[0]
    parts = [pl.ds(i * rows // STORES, rows // STORES) for i in range(STORES)]
    copies = [
        pltpu.make_async_copy(source.at[part], target.at[part], sem.at[k, i])
        for k, (source, target) in enumerate([(mixed, mixed_hbm), (attended, attended_hbm)])
        for i, part in enumerate(parts)
    ]
    for copy in copies:
        copy.start()
    for copy in copies:
        copy.wait()


def on_device(
    n,
    mp,
    stream,
    norm_gain,
    short_outer,
    short_inner,
    short_filter,
    long_outer,
    long_inner,
    long_decay,
    query_heads,
    key_heads,
):
    rows, width = stream.shape
    wide = width // CHUNKS
    heads = wide // HEAD_DIM
    groups = n // GROUP
    bf16, f32 = jnp.bfloat16, jnp.float32
    anywhere = pl.BlockSpec(memory_space=pltpu.HBM)
    vmem = pl.BlockSpec(memory_space=pltpu.VMEM)
    dma = pltpu.SemaphoreType.DMA

    def in_hbm(array):
        return pltpu.with_memory_space_constraint(array, pltpu.HBM)

    mixed, attended = pl.pallas_call(
        functools.partial(kernel, n, mp, float(width * mp)),
        out_shape=[jax.ShapeDtypeStruct((rows, width), bf16)] * 2,
        in_specs=[anywhere] * 11,
        out_specs=[vmem] * 2,
        scratch_shapes=[
            pltpu.VMEM((2, 1, width), f32),
            pltpu.VMEM((7, rows, width), bf16),
            pltpu.VMEM((3 * rows, 2 * rows), bf16),
        ]
        + [pltpu.VMEM((CHUNKS, 2 * rows, wide), bf16)] * 3
        + [pltpu.VMEM((CHUNKS + HALF + 1, rows, wide), bf16)]
        + [pltpu.VMEM((rows, wide), bf16)] * 2
        + [pltpu.VMEM((rows, wide), f32)] * 2
        + [pltpu.VMEM((rows, width), f32)] * 3
        + [
            pltpu.VMEM((2 * rows, width), f32),
            pltpu.VMEM((CHUNKS, heads, rows, 2 * rows), bf16),
            pltpu.VMEM((heads, rows, rows), bf16),
        ]
        + [pltpu.VMEM((2 * heads, rows), f32)] * 2
        + [
            pltpu.VMEM((8, rows), f32),
            pltpu.VMEM((mp - 1, 8, rows), f32),
        ]
        + [pltpu.VMEM((CHUNKS, 1, wide), f32)] * 8
        + [
            pltpu.VMEM((CHUNKS, groups, 1, wide), f32),
            dma((8,)),
            dma((CHUNKS,)),
            dma((mp - 1,)),
            dma((mp - 1,)),
        ]
        + [dma((1,)), dma((CHUNKS,))] * 3
        + [dma((2,)), dma((CHUNKS + HALF + 1,))]
        + [dma((1,)), dma((CHUNKS,))]
        + [dma((groups,)), dma((CHUNKS,))]
        + [dma((2,))] * 2,
        compiler_params=pltpu.CompilerParams(
            collective_id=0, has_side_effects=True, vmem_limit_bytes=51 * 1024 * 1024
        ),
    )(
        in_hbm(norm_gain.reshape(1, width)),
        in_hbm(long_decay.reshape(1, width)),
        in_hbm(jnp.asarray(waves_of(rows), bf16)),
        stream,
        short_outer,
        short_inner,
        short_filter,
        long_outer,
        long_inner,
        query_heads,
        key_heads,
    )
    return pl.pallas_call(
        store,
        out_shape=[jax.ShapeDtypeStruct((rows, width), bf16)] * 2,
        in_specs=[vmem] * 2,
        out_specs=[anywhere] * 2,
        scratch_shapes=[dma((2, STORES))],
        compiler_params=pltpu.CompilerParams(vmem_limit_bytes=1024 * 1024),
    )(mixed, attended)


def solution(mesh):
    return jax.shard_map(
        functools.partial(on_device, mesh.shape["seq"], mesh.shape["mp"]),
        mesh=mesh,
        in_specs=(
            P("seq", "mp"),
            P("mp"),
            P("seq", "mp"),
            P("seq", "mp"),
            P(None, "mp"),
            P("seq", "mp"),
            P("seq", "mp"),
            P("mp"),
            P("seq", "mp"),
            P("seq", "mp"),
        ),
        out_specs=(P("seq", "mp"), P("seq", "mp")),
        check_vma=False,
    )
```

```python
import functools

import jax
import jax.numpy as jnp
import numpy as np
from jax import lax
from jax.experimental import pallas as pl
from jax.experimental.pallas import tpu as pltpu
from jax.sharding import PartitionSpec as P

HEAD_DIM = 128
CHUNKS = 4
HALF = CHUNKS // 2
LENT = CHUNKS - 1
KEPT = 2
GROUP = 4
TILE = 256
STORES = 2
MESH = pl.DeviceIdType.MESH


def wave(frequency, place, rows):
    shift = np.where(frequency >= rows, rows, 0)
    index = ((2 * (frequency % rows) + 1) * place + shift) % (4 * rows)
    return np.cos(index * (np.pi / (2 * rows)))


def waves_of(rows):
    every = np.arange(2 * rows)
    fwd = wave(every[:, None], every[None, :], rows)
    inv = wave(every[None, :], every[:rows, None] + rows, rows) / rows
    return np.concatenate([fwd, inv], axis=0)


def dot(a, b):
    return jnp.dot(a, b, preferred_element_type=jnp.float32)


def dot_nt(a, b):
    return lax.dot_general(a, b, (((1,), (1,)), ((), ())), preferred_element_type=jnp.float32)


def dot_tn(a, b):
    return lax.dot_general(a, b, (((0,), (0,)), ((), ())), preferred_element_type=jnp.float32)


def kernel(
    n,
    mp,
    channels,
    gain_hbm,
    decay_hbm,
    waves_hbm,
    stream_hbm,
    souter_hbm,
    sinner_hbm,
    filt_hbm,
    louter_hbm,
    linner_hbm,
    query_hbm,
    key_hbm,
    mixed,
    attended,
    vectors,
    blocks,
    waves,
    keys,
    values,
    ext,
    relayed,
    next_query,
    lent,
    own_part,
    shares,
    power,
    inv_power,
    cum,
    spectrum,
    weights,
    lent_weights,
    stats,
    stats_in,
    squares,
    squares_in,
    own_state,
    member_state,
    pair_state,
    before_state,
    group_state,
    next_state,
    across_state,
    carry_in,
    states,
    load_sem,
    key_sem,
    sq_send,
    sq_recv,
    k_send,
    k_recv,
    t_send,
    t_recv,
    v_send,
    v_recv,
    cross_send,
    cross_recv,
    state_send,
    state_recv,
    e_send,
    e_recv,
    lend_send,
    lend_recv,
):
    gain_ref, decay_ref = vectors.at[0], vectors.at[1]
    stream, sinner, filt, souter, linner, louter, query = (blocks.at[i] for i in range(7))
    me = lax.axis_index("seq")
    col = lax.axis_index("mp")
    rows, width = stream.shape
    fwd, inv = waves.at[pl.ds(0, 2 * rows)], waves.at[pl.ds(2 * rows, rows)]
    wide = width // CHUNKS
    tiles = wide // TILE
    heads = wide // HEAD_DIM
    keep = KEPT * HEAD_DIM
    has_next = me < n - 1
    has_prev = me > 0
    groups = n // GROUP
    group = me // GROUP
    role = lax.rem(me, GROUP)
    later = groups - 1 - group
    first = role == 0
    lends = role == 1
    borrows = role == 2
    relays = jnp.logical_and(role == 3, later > 0)
    forwards = jnp.logical_and(lends, later > 0)
    even = lax.rem(me, 2) == 0
    own = pl.ds(rows, rows)
    before = pl.ds(0, rows)

    def seq(target):
        return {"seq": lax.rem(target + n, n)}

    barrier = pltpu.get_barrier_semaphore()

    def greet(target, when):
        @pl.when(when)
        def _():
            pl.semaphore_signal(barrier, inc=1, device_id=seq(target), device_id_type=MESH)

    greet(me + 1, has_next)
    greet(me - 1, has_prev)
    greet(me - 2, borrows)
    greet(me + 2, forwards)
    greet(me - 3, jnp.logical_and(first, group > 0))

    @pl.when(first)
    def _():
        def greet_earlier(j, _):
            pl.semaphore_signal(
                barrier, inc=1, device_id=seq(j * GROUP + 2), device_id_type=MESH
            )
            return 0

        lax.fori_loop(0, group, greet_earlier, 0)

    greeted = has_next.astype(jnp.int32) + has_prev.astype(jnp.int32) + mp - 1
    greeted += jnp.where(borrows, later, 0)
    greeted += (first | relays | forwards).astype(jnp.int32)

    for k in range(1, mp):
        pl.semaphore_signal(
            barrier, inc=1, device_id={"mp": lax.rem(col + k, mp)}, device_id_type=MESH
        )

    def load(source, target, sem):
        pltpu.make_async_copy(source, target, sem).start()

    def landed(buffer, sem):
        pltpu.make_async_copy(buffer, buffer, sem).wait()

    def load_key(c, sem):
        load(key_hbm.at[:, pl.ds(c * wide, wide)], keys.at[c, own], sem)

    last = pl.ds(LENT * wide + keep, wide - keep)
    rest = pl.ds(0, LENT * wide + keep)
    load(query_hbm.at[:, last], query.at[:, last], load_sem.at[6])
    load_key(0, key_sem.at[0])
    load_key(HALF, key_sem.at[1])
    load(stream_hbm, stream, load_sem.at[0])
    load(gain_hbm, gain_ref, load_sem.at[2])
    load(decay_hbm, decay_ref, load_sem.at[2])

    def remote(source, target, send, recv, device):
        return pltpu.make_async_remote_copy(
            src_ref=source,
            dst_ref=target,
            send_sem=send,
            recv_sem=recv,
            device_id=device,
            device_id_type=MESH,
        )

    def to_next(buffer, c, send, recv):
        return remote(
            buffer.at[c, own], buffer.at[c, before], send.at[0], recv.at[c], seq(me + 1)
        )

    def to_relay(buffer, c, slot, send):
        return remote(
            buffer.at[c, own], relayed.at[slot], send.at[0], cross_recv.at[slot], seq(me - 2)
        )

    k_copies = [to_next(keys, c, k_send, k_recv) for c in range(CHUNKS)]
    t_copies = [to_next(ext, c, t_send, t_recv) for c in range(CHUNKS)]
    v_copies = [to_next(values, c, v_send, v_recv) for c in range(CHUNKS)]
    lent_query = remote(
        query.at[:, last], next_query, lend_send.at[0], lend_recv.at[0], seq(me - 1)
    )
    lent_stats = remote(stats, stats_in, lend_send.at[1], lend_recv.at[1], seq(me + 1))
    lent_values = remote(
        lent,
        values.at[LENT, before, pl.ds(keep, wide - keep)],
        lend_send.at[4],
        v_recv.at[CHUNKS],
        seq(me + 1),
    )

    def kept(buffer, send, recv):
        part = pl.ds(0, keep)
        return remote(
            buffer.at[LENT, own, part],
            buffer.at[LENT, before, part],
            send,
            recv.at[LENT],
            seq(me + 1),
        )

    kept_keys = kept(keys, lend_send.at[2], k_recv)
    kept_values = kept(values, lend_send.at[3], v_recv)

    key_relay = [
        later > 1 if c >= HALF else True for c in range(CHUNKS)
    ]
    tail_relay = group == 0
    key_slot = [(c + HALF) % CHUNKS for c in range(CHUNKS)]

    def send_key(c, when=True):
        relay = jnp.logical_and(relays, key_relay[c])
        direct = jnp.logical_and(has_next, jnp.logical_not(relay))
        if c == LENT:
            direct = jnp.logical_and(direct, jnp.logical_not(lends))

            @pl.when(lends)
            def _():
                kept_keys.start()

        @pl.when(jnp.logical_and(relay, when))
        def _():
            to_relay(keys, c, key_slot[c], k_send).start()

        @pl.when(jnp.logical_and(direct, when))
        def _():
            k_copies[c].start()

    def send_tail(c):
        direct = has_next
        if c >= HALF:
            relay = jnp.logical_and(relays, tail_relay)
            direct = jnp.logical_and(has_next, jnp.logical_not(relay))

            @pl.when(relay)
            def _():
                to_relay(ext, c, CHUNKS + c - HALF, t_send).start()

        @pl.when(direct)
        def _():
            t_copies[c].start()

    def pass_on(buffer, c, slot, recv, when):
        @pl.when(jnp.logical_and(forwards, when))
        def _():
            remote(
                buffer.at[c, own], relayed.at[slot], k_send.at[0], cross_recv.at[slot], seq(me + 2)
            ).wait_recv()
            remote(
                relayed.at[slot], buffer.at[c, before], cross_send.at[0], recv.at[c], seq(me + 3)
            ).start()

    def pass_key(c):
        pass_on(keys, c, key_slot[c], k_recv, key_relay[c])

    def pass_tail(c):
        pass_on(ext, c, CHUNKS + c - HALF, t_recv, tail_relay)

    def pass_value():
        pass_on(values, 0, CHUNKS + HALF, v_recv, tail_relay)

    @pl.when(me == 0)
    def _():
        for c in range(CHUNKS):
            keys[c, :rows, :] = jnp.zeros((rows, wide), keys.dtype)
            values[c, :rows, :] = jnp.zeros((rows, wide), values.dtype)
            ext[c, :rows, :] = jnp.zeros((rows, wide), ext.dtype)

    pl.semaphore_wait(barrier, greeted)
    origin = group == 0
    late = jnp.logical_and(relays, origin)
    landed(query.at[:, last], load_sem.at[6])

    @pl.when(jnp.logical_and(borrows, jnp.logical_not(origin)))
    def _():
        lent_query.start()

    landed(keys.at[0, own], key_sem.at[0])
    send_key(0, jnp.logical_not(late))
    ahead = jnp.logical_and(relays, later == 1)
    landed(keys.at[HALF, own], key_sem.at[1])
    send_key(HALF, ahead)
    load(waves_hbm, waves, load_sem.at[3])
    load(filt_hbm, filt, load_sem.at[4])
    load(sinner_hbm, sinner, load_sem.at[1])
    others = [c for c in range(1, CHUNKS) if c != HALF]
    for i, c in enumerate(others):
        load_key(c, key_sem.at[2 + i])
    load(souter_hbm, souter, load_sem.at[5])
    load(linner_hbm, linner, load_sem.at[5])
    load(louter_hbm, louter, load_sem.at[5])
    load(query_hbm.at[:, rest], query.at[:, rest], load_sem.at[7])
    landed(stream, load_sem.at[0])

    def square(i, acc):
        x = stream[:, pl.ds(pl.multiple_of(i * 128, 128), 128)].astype(jnp.float32)
        return acc + x * x

    total = lax.fori_loop(
        0, width // 128, square, jnp.zeros((rows, 128), jnp.float32), unroll=4
    )
    squares[...] = jnp.sum(total.T.reshape(128 // 8, 8, rows), axis=0)
    sq_copies = [
        pltpu.make_async_remote_copy(
            src_ref=squares,
            dst_ref=squares_in.at[k - 1],
            send_sem=sq_send.at[k - 1],
            recv_sem=sq_recv.at[k - 1],
            device_id={"mp": lax.rem(col + k, mp)},
            device_id_type=MESH,
        )
        for k in range(1, mp)
    ]
    for copy in sq_copies:
        copy.start()

    landed(vectors, load_sem.at[2])
    step = lax.broadcasted_iota(jnp.int32, (rows, TILE), 0).astype(jnp.float32)

    def powers(i, _):
        cols = pl.ds(pl.multiple_of(i * TILE, TILE), TILE)
        exponent = step * decay_ref[:, cols]
        power[:, cols] = jnp.exp(-exponent)
        inv_power[:, cols] = jnp.exp(exponent)
        return 0

    lax.fori_loop(0, width // TILE, powers, 0)
    landed(waves, load_sem.at[3])
    landed(filt, load_sem.at[4])

    def spectra(i, _):
        cols = pl.ds(pl.multiple_of(i * TILE, TILE), TILE)
        spectrum[:, cols] = dot(fwd[:, :rows], filt[:, cols])
        return 0

    lax.fori_loop(0, width // TILE // 2, spectra, 0)
    landed(sinner, load_sem.at[1])
    total = squares[...]
    for k, copy in enumerate(sq_copies):
        copy.wait_recv()
        total = total + squares_in[k]
    mean_square = jnp.sum(total, axis=0, keepdims=True) / channels
    norm = jnp.broadcast_to(1.0 / jnp.sqrt(mean_square + 0.5), (128, rows)).T
    norm = jnp.concatenate([norm] * (TILE // 128), axis=1)

    for c in range(CHUNKS):

        def short(i, _, c=c):
            cols = pl.ds(pl.multiple_of(c * wide + i * TILE, TILE), TILE)
            x = stream[:, cols].astype(jnp.float32) * gain_ref[:, cols] * norm
            ext[c, own, pl.ds(pl.multiple_of(i * TILE, TILE), TILE)] = (
                sinner[:, cols].astype(jnp.float32) * x
            ).astype(jnp.bfloat16)
            return 0

        lax.fori_loop(0, tiles, short, 0)
        send_tail(c)

    for i, c in enumerate(others):
        landed(keys.at[c, own], key_sem.at[2 + i])
    send_key(0, late)
    for c in range(1, CHUNKS):
        send_key(c, jnp.logical_not(ahead) if c == HALF else True)

    lax.fori_loop(width // TILE // 2, width // TILE, spectra, 0)
    landed(blocks.at[pl.ds(3, 3)], load_sem.at[5])
    row = lax.broadcasted_iota(jnp.int32, (rows, 2 * rows), 0)
    column = lax.broadcasted_iota(jnp.int32, (rows, 2 * rows), 1)
    lower = (jnp.where(column >= rows, column - rows, column) <= row).astype(
        jnp.float32
    ).astype(jnp.bfloat16)

    def state_copy(c, target):
        return remote(
            group_state.at[c],
            states.at[c, group],
            e_send.at[target],
            e_recv.at[c],
            seq(target * GROUP),
        )

    def mix_chunk(c):
        @pl.when(has_prev)
        def _():
            t_copies[c].wait_recv()

        def mix(i, _):
            here = pl.ds(pl.multiple_of(i * TILE, TILE), TILE)
            cols = pl.ds(pl.multiple_of(c * wide + i * TILE, TILE), TILE)
            x = dot(fwd[...], ext[c, :, here])
            x_re, x_im = x[:rows], x[rows:]
            h_re, h_im = spectrum[:rows, cols], spectrum[rows:, cols]
            y = jnp.concatenate(
                [x_re * h_re - x_im * h_im, x_re * h_im + x_im * h_re], axis=0
            ).astype(jnp.bfloat16)
            conv = dot(inv[...], y)
            long_in = (
                linner[:, cols].astype(jnp.float32) * souter[:, cols].astype(jnp.float32) * conv
            ).astype(jnp.bfloat16)
            v = long_in.astype(jnp.float32) * inv_power[:, cols]
            high = v.astype(jnp.bfloat16)
            low = (v - high.astype(jnp.float32)).astype(jnp.bfloat16)
            sums = dot(lower, jnp.concatenate([high, low], axis=0))
            cum[:, cols] = sums
            own_state[c, :, here] = sums[rows - 1 :] * power[rows - 1 :, cols]
            return 0

        lax.fori_loop(0, tiles, mix, 0)

        @pl.when(jnp.logical_not(even))
        def _():
            remote(
                own_state.at[c], member_state.at[c], state_send.at[0], state_recv.at[c], seq(me - 1)
            ).start()

    def rate_of(c):
        return decay_ref[:, pl.ds(c * wide, wide)]

    def pair(c):
        @pl.when(first)
        def _():
            landed(member_state.at[c], state_recv.at[c])
            over = jnp.exp(-rate_of(c) * rows)
            pair_state[c] = own_state[c] * over + member_state[c]
            remote(
                pair_state.at[c], before_state.at[c], cross_send.at[0], cross_recv.at[c], seq(me + 2)
            ).start()

    def collect(c):
        @pl.when(borrows)
        def _():
            landed(member_state.at[c], state_recv.at[c])
            landed(before_state.at[c], cross_recv.at[c])
            over = jnp.exp(-rate_of(c) * rows)
            group_state[c] = (before_state[c] * over + own_state[c]) * over + member_state[c]

            def send_state(target, _):
                state_copy(c, target).start()
                return 0

            lax.fori_loop(group + 1, groups, send_state, 0)

    def spread(c):
        @pl.when(first)
        def _():
            for g in range(1, groups):

                @pl.when(group == g)
                def _(g=g):
                    landed(states.at[c, pl.ds(0, g)], e_recv.at[c])

            over_group = jnp.exp(-rate_of(c) * (rows * GROUP))

            def arrive(j, state):
                return state * over_group + states[c, j]

            state = lax.fori_loop(0, group, arrive, jnp.zeros((1, wide), jnp.float32))
            over = jnp.exp(-rate_of(c) * rows)
            carry_in[c] = state
            next_state[c] = state * over + own_state[c]
            give_next(c)
            across_state[c] = state * jnp.exp(-rate_of(c) * (2 * rows)) + pair_state[c]
            remote(
                across_state.at[c], carry_in.at[c], cross_send.at[1], e_recv.at[c], seq(me + 2)
            ).start()

    def give_next(c):
        remote(
            next_state.at[c], carry_in.at[c], state_send.at[0], state_recv.at[c], seq(me + 1)
        ).start()

    def hand_on(c):
        @pl.when(borrows)
        def _():
            landed(carry_in.at[c], e_recv.at[c])
            next_state[c] = carry_in[c] * jnp.exp(-rate_of(c) * rows) + own_state[c]
            give_next(c)

    def long_chunk(c):
        @pl.when(jnp.logical_not(even))
        def _():
            landed(carry_in.at[c], state_recv.at[c])

        rate = rate_of(c)
        carried = carry_in[c] * jnp.exp(-rate)
        z = 2.0 * rate
        scale = jnp.sqrt(jnp.tanh(0.5 * z) * (1.0 + jnp.exp(-z)))
        for i in range(tiles):
            here = pl.ds(i * TILE, TILE)
            cols = pl.ds(c * wide + i * TILE, TILE)
            part = slice(i * TILE, (i + 1) * TILE)
            conv = (cum[:, cols] + carried[:, part]) * power[:, cols]
            out = (
                louter[:, cols].astype(jnp.float32) * (conv * scale[:, part])
            ).astype(jnp.bfloat16)
            values[c, own, here] = out
            mixed[:, cols] = out

        direct = has_next
        if c == LENT:
            direct = jnp.logical_and(has_next, jnp.logical_not(lends))

            @pl.when(lends)
            def _():
                kept_values.start()

                def lend_values(h, _):
                    here = pl.ds(pl.multiple_of(h * HEAD_DIM, HEAD_DIM), HEAD_DIM)
                    there = pl.ds(pl.multiple_of(keep + h * HEAD_DIM, HEAD_DIM), HEAD_DIM)
                    lent[:, here] = dot_tn(
                        lent_weights[h], values[LENT, own, there]
                    ).astype(jnp.bfloat16)
                    return 0

                lax.fori_loop(0, heads - KEPT, lend_values, 0, unroll=heads - KEPT)
                lent_values.start()

        if c == 0:
            relay = jnp.logical_and(relays, group == 0)
            direct = jnp.logical_and(has_next, jnp.logical_not(relay))

            @pl.when(relay)
            def _():
                to_relay(values, c, CHUNKS + HALF, v_send).start()

        if c == 0:
            direct = jnp.logical_and(direct, jnp.logical_not(held))

        @pl.when(direct)
        def _():
            v_copies[c].start()

    def lend_weights():
        @pl.when(lends)
        def _():
            lent_query.wait_recv()
            stats[...] = jnp.ones(stats.shape, stats.dtype)
            for h in range(heads - KEPT):
                here = pl.ds(h * HEAD_DIM, HEAD_DIM)
                there = pl.ds(keep + h * HEAD_DIM, HEAD_DIM)
                s = dot_nt(keys[LENT, own, there], next_query[:, here]) * HEAD_DIM ** (-0.5)
                top = jnp.max(s, axis=0, keepdims=True)
                e = jnp.exp(s - top)
                total = jnp.sum(e, axis=0, keepdims=True)
                lent_weights[h] = (e * (1.0 / total)).astype(jnp.bfloat16)
                stats[h : h + 1, :] = top
                stats[heads + h : heads + h + 1, :] = total
            lent_stats.start()

    valid = (column <= row + rows) & ((column >= rows) | has_prev)

    def score_chunk(c, when=True, half=None):
        if c == LENT:
            when = jnp.logical_not(borrows)

            @pl.when(borrows)
            def _():
                kept_keys.wait_recv()

        @pl.when(jnp.logical_and(has_prev, when if half != 1 else False))
        def _():
            k_copies[c].wait_recv()

        def score(h, _):
            here = pl.ds(pl.multiple_of(h * HEAD_DIM, HEAD_DIM), HEAD_DIM)
            cols = pl.ds(pl.multiple_of(c * wide + h * HEAD_DIM, HEAD_DIM), HEAD_DIM)
            s = dot_nt(query[:, cols], keys[c, :, here]) * HEAD_DIM ** (-0.5)
            s = jnp.where(valid, s, -1e30)
            e = jnp.exp(s - jnp.max(s, axis=1, keepdims=True))
            e = e * (1.0 / jnp.sum(e, axis=1, keepdims=True))
            weights[c, h] = e.astype(jnp.bfloat16)
            return 0

        start = 2 if half == 1 else 0
        stop = 2 if half == 0 else heads

        def run():
            lax.fori_loop(start, stop, score, 0, unroll=2)

        if when is True:
            run()
        else:
            pl.when(when)(run)
        if c == LENT:

            @pl.when(borrows)
            def _():
                lax.fori_loop(0, KEPT, score, 0, unroll=2)

    def borrow():
        @pl.when(borrows)
        def _():
            upper = lax.broadcasted_iota(
                jnp.int32, (rows, rows), 0
            ) <= lax.broadcasted_iota(jnp.int32, (rows, rows), 1)
            stats[...] = jnp.ones(stats.shape, stats.dtype)
            for h in range(heads - KEPT):
                here = pl.ds(keep + h * HEAD_DIM, HEAD_DIM)
                cols = pl.ds(LENT * wide + keep + h * HEAD_DIM, HEAD_DIM)
                s = dot_nt(keys[LENT, own, here], query[:, cols]) * HEAD_DIM ** (-0.5)
                s = jnp.where(upper, s, -1e30)
                top = jnp.max(s, axis=0, keepdims=True)
                e = jnp.exp(s - top)
                lent_weights[h] = e.astype(jnp.bfloat16)
                stats[h : h + 1, :] = top
                stats[heads + h : heads + h + 1, :] = jnp.sum(e, axis=0, keepdims=True)
            for h in range(heads - KEPT):
                here = pl.ds(keep + h * HEAD_DIM, HEAD_DIM)
                own_part[:, here] = dot_tn(lent_weights[h], values[LENT, own, here])

    def blend():
        @pl.when(borrows)
        def _():
            lent_stats.wait_recv()
            top, total = stats[:heads], stats[heads:]
            top_before, total_before = stats_in[:heads], stats_in[heads:]
            most = jnp.maximum(top, top_before)
            here_scale = jnp.exp(top - most)
            before_scale = jnp.exp(top_before - most) * total_before
            inverse = 1.0 / (total * here_scale + before_scale)
            both = jnp.concatenate([here_scale * inverse, before_scale * inverse], axis=0)
            both = jnp.concatenate(
                [both, jnp.zeros((HEAD_DIM - 2 * heads, rows), jnp.float32)], axis=0
            ).T
            for h in range(heads - KEPT):
                here = pl.ds(keep + h * HEAD_DIM, HEAD_DIM)
                own_part[:, here] = own_part[:, here] * both[:, h : h + 1]
                shares[:, here] = jnp.broadcast_to(
                    both[:, heads + h : heads + h + 1], (rows, HEAD_DIM)
                )

    def attend_chunk(c):
        when = has_prev
        if c == LENT:
            when = jnp.logical_and(has_prev, jnp.logical_not(borrows))

        @pl.when(when)
        def _():
            v_copies[c].wait_recv()

        def gather(h, _):
            here = pl.ds(pl.multiple_of(h * HEAD_DIM, HEAD_DIM), HEAD_DIM)
            cols = pl.ds(pl.multiple_of(c * wide + h * HEAD_DIM, HEAD_DIM), HEAD_DIM)
            attended[:, cols] = dot(weights[c, h], values[c, :, here]).astype(jnp.bfloat16)
            return 0

        def finish():
            lax.fori_loop(0, heads, gather, 0, unroll=8)

        if c < LENT:
            finish()
            return
        pl.when(jnp.logical_not(borrows))(finish)

        @pl.when(borrows)
        def _():
            kept_values.wait_recv()
            lax.fori_loop(0, KEPT, gather, 0, unroll=KEPT)
            lent_values.wait_recv()
            for i in range(keep // TILE, tiles):
                here = pl.ds(i * TILE, TILE)
                cols = pl.ds(c * wide + i * TILE, TILE)
                attended[:, cols] = (
                    own_part[:, here]
                    + shares[:, here] * values[c, before, here].astype(jnp.float32)
                ).astype(jnp.bfloat16)

    mix_chunk(0)
    pair(0)
    pass_tail(2)
    mix_chunk(1)
    pair(1)
    collect(0)

    @pl.when(jnp.logical_and(borrows, origin))
    def _():
        lent_query.start()

    pass_tail(3)
    mix_chunk(2)
    pair(2)
    collect(1)
    landed(query.at[:, rest], load_sem.at[7])
    spread(0)
    mix_chunk(3)
    pair(3)
    collect(2)
    spread(1)
    pass_key(0)
    hand_on(0)
    held = relays & (group > 0)
    long_chunk(0)
    score_chunk(0, jnp.logical_not(first), 0)

    @pl.when(held)
    def _():
        v_copies[0].start()

    score_chunk(0, jnp.logical_not(first), 1)
    collect(3)
    spread(2)
    hand_on(1)
    long_chunk(1)
    pass_key(1)
    pass_key(2)
    hand_on(2)
    long_chunk(2)
    lend_weights()
    pass_key(3)
    score_chunk(1, jnp.logical_not(first))
    spread(3)
    hand_on(3)
    long_chunk(3)
    pass_value()
    score_chunk(0, first)
    score_chunk(1, first)
    score_chunk(2)
    score_chunk(3)
    borrow()
    for c in range(CHUNKS - 1):
        attend_chunk(c)
    blend()
    attend_chunk(LENT)

    for copy in sq_copies:
        copy.wait_send()

    def sent(buffer, sem):
        pltpu.make_async_copy(buffer, buffer, sem).wait()

    @pl.when(jnp.logical_not(even))
    def _():
        sent(own_state, state_send.at[0])

    @pl.when(even)
    def _():
        sent(next_state, state_send.at[0])

    @pl.when(first)
    def _():
        sent(pair_state, cross_send.at[0])
        sent(across_state, cross_send.at[1])

    @pl.when(borrows)
    def _():
        lent_query.wait_send()

        def all_sent(target, _):
            sent(group_state, e_send.at[target])
            return 0

        lax.fori_loop(group + 1, groups, all_sent, 0)

    for tails in (True, False):
        for fewer in (True, False):
            slots = pl.ds(HALF if fewer else 0, CHUNKS + tails * (HALF + 1) - fewer * HALF)

            @pl.when(forwards & (tail_relay == tails) & ((later == 1) == fewer))
            def _(slots=slots):
                sent(relayed.at[slots], cross_send.at[0])

    @pl.when(lends)
    def _():
        sent(keys.at[pl.ds(0, LENT), own], k_send.at[0])
        sent(ext.at[:, own], t_send.at[0])
        sent(values.at[pl.ds(0, LENT), own], v_send.at[0])
        lent_stats.wait_send()
        kept_keys.wait_send()
        kept_values.wait_send()
        lent_values.wait_send()

    @pl.when(jnp.logical_and(has_next, jnp.logical_not(lends)))
    def _():
        sent(keys.at[:, own], k_send.at[0])
        sent(ext.at[:, own], t_send.at[0])
        sent(values.at[:, own], v_send.at[0])


def store(mixed, attended, mixed_hbm, attended_hbm, sem):
    rows = mixed.shape[0]
    parts = [pl.ds(i * rows // STORES, rows // STORES) for i in range(STORES)]
    copies = [
        pltpu.make_async_copy(source.at[part], target.at[part], sem.at[k, i])
        for k, (source, target) in enumerate([(mixed, mixed_hbm), (attended, attended_hbm)])
        for i, part in enumerate(parts)
    ]
    for copy in copies:
        copy.start()
    for copy in copies:
        copy.wait()


def on_device(
    n,
    mp,
    stream,
    norm_gain,
    short_outer,
    short_inner,
    short_filter,
    long_outer,
    long_inner,
    long_decay,
    query_heads,
    key_heads,
):
    rows, width = stream.shape
    wide = width // CHUNKS
    heads = wide // HEAD_DIM
    groups = n // GROUP
    bf16, f32 = jnp.bfloat16, jnp.float32
    anywhere = pl.BlockSpec(memory_space=pltpu.HBM)
    vmem = pl.BlockSpec(memory_space=pltpu.VMEM)
    dma = pltpu.SemaphoreType.DMA

    def in_hbm(array):
        return pltpu.with_memory_space_constraint(array, pltpu.HBM)

    mixed, attended = pl.pallas_call(
        functools.partial(kernel, n, mp, float(width * mp)),
        out_shape=[jax.ShapeDtypeStruct((rows, width), bf16)] * 2,
        in_specs=[anywhere] * 11,
        out_specs=[vmem] * 2,
        scratch_shapes=[
            pltpu.VMEM((2, 1, width), f32),
            pltpu.VMEM((7, rows, width), bf16),
            pltpu.VMEM((3 * rows, 2 * rows), bf16),
        ]
        + [pltpu.VMEM((CHUNKS, 2 * rows, wide), bf16)] * 3
        + [pltpu.VMEM((CHUNKS + HALF + 1, rows, wide), bf16)]
        + [pltpu.VMEM((rows, wide - KEPT * HEAD_DIM), bf16)] * 2
        + [pltpu.VMEM((rows, wide), f32)] * 2
        + [pltpu.VMEM((rows, width), f32)] * 3
        + [
            pltpu.VMEM((2 * rows, width), f32),
            pltpu.VMEM((CHUNKS, heads, rows, 2 * rows), bf16),
            pltpu.VMEM((heads, rows, rows), bf16),
        ]
        + [pltpu.VMEM((2 * heads, rows), f32)] * 2
        + [
            pltpu.VMEM((8, rows), f32),
            pltpu.VMEM((mp - 1, 8, rows), f32),
        ]
        + [pltpu.VMEM((CHUNKS, 1, wide), f32)] * 8
        + [
            pltpu.VMEM((CHUNKS, groups, 1, wide), f32),
            dma((8,)),
            dma((CHUNKS,)),
            dma((mp - 1,)),
            dma((mp - 1,)),
        ]
        + [dma((1,)), dma((CHUNKS,))] * 2
        + [dma((1,)), dma((CHUNKS + 1,))]
        + [dma((2,)), dma((CHUNKS + HALF + 1,))]
        + [dma((1,)), dma((CHUNKS,))]
        + [dma((groups,)), dma((CHUNKS,))]
        + [dma((5,)), dma((2,))],
        compiler_params=pltpu.CompilerParams(
            collective_id=0, has_side_effects=True, vmem_limit_bytes=51 * 1024 * 1024
        ),
    )(
        in_hbm(norm_gain.reshape(1, width)),
        in_hbm(long_decay.reshape(1, width)),
        in_hbm(jnp.asarray(waves_of(rows), bf16)),
        stream,
        short_outer,
        short_inner,
        short_filter,
        long_outer,
        long_inner,
        query_heads,
        key_heads,
    )
    return pl.pallas_call(
        store,
        out_shape=[jax.ShapeDtypeStruct((rows, width), bf16)] * 2,
        in_specs=[vmem] * 2,
        out_specs=[anywhere] * 2,
        scratch_shapes=[dma((2, STORES))],
        compiler_params=pltpu.CompilerParams(vmem_limit_bytes=1024 * 1024),
    )(mixed, attended)


def solution(mesh):
    return jax.shard_map(
        functools.partial(on_device, mesh.shape["seq"], mesh.shape["mp"]),
        mesh=mesh,
        in_specs=(
            P("seq", "mp"),
            P("mp"),
            P("seq", "mp"),
            P("seq", "mp"),
            P(None, "mp"),
            P("seq", "mp"),
            P("seq", "mp"),
            P("mp"),
            P("seq", "mp"),
            P("seq", "mp"),
        ),
        out_specs=(P("seq", "mp"), P("seq", "mp")),
        check_vma=False,
    )
```

```python
import functools

import jax
import jax.numpy as jnp
import numpy as np
from jax import lax
from jax.experimental import pallas as pl
from jax.experimental.pallas import tpu as pltpu
from jax.sharding import PartitionSpec as P

HEAD_DIM = 128
CHUNKS = 4
HALF = CHUNKS // 2
LENT = CHUNKS - 1
KEPT = 2
GROUP = 4
TILE = 256
STORES = 2
MESH = pl.DeviceIdType.MESH


def wave(frequency, place, rows):
    shift = np.where(frequency >= rows, rows, 0)
    index = ((2 * (frequency % rows) + 1) * place + shift) % (4 * rows)
    return np.cos(index * (np.pi / (2 * rows)))


def waves_of(rows):
    every = np.arange(2 * rows)
    fwd = wave(every[:, None], every[None, :], rows)
    inv = wave(every[None, :], every[:rows, None] + rows, rows) / rows
    return np.concatenate([fwd, inv], axis=0)


def dot(a, b):
    return jnp.dot(a, b, preferred_element_type=jnp.float32)


def dot_nt(a, b):
    return lax.dot_general(a, b, (((1,), (1,)), ((), ())), preferred_element_type=jnp.float32)


def dot_tn(a, b):
    return lax.dot_general(a, b, (((0,), (0,)), ((), ())), preferred_element_type=jnp.float32)


def kernel(
    n,
    mp,
    channels,
    gain_hbm,
    decay_hbm,
    waves_hbm,
    stream_hbm,
    souter_hbm,
    sinner_hbm,
    filt_hbm,
    louter_hbm,
    linner_hbm,
    query_hbm,
    key_hbm,
    mixed,
    attended,
    vectors,
    blocks,
    waves,
    keys,
    values,
    ext,
    relayed,
    next_query,
    lent,
    own_part,
    shares,
    power,
    inv_power,
    cum,
    spectrum,
    weights,
    lent_weights,
    stats,
    stats_in,
    squares,
    squares_in,
    own_state,
    member_state,
    pair_state,
    before_state,
    group_state,
    next_state,
    across_state,
    carry_in,
    states,
    load_sem,
    key_sem,
    sq_send,
    sq_recv,
    k_send,
    k_recv,
    t_send,
    t_recv,
    v_send,
    v_recv,
    cross_send,
    cross_recv,
    state_send,
    state_recv,
    e_send,
    e_recv,
    lend_send,
    lend_recv,
):
    gain_ref, decay_ref = vectors.at[0], vectors.at[1]
    stream, sinner, filt, souter, linner, louter, query = (blocks.at[i] for i in range(7))
    me = lax.axis_index("seq")
    col = lax.axis_index("mp")
    rows, width = stream.shape
    fwd, inv = waves.at[pl.ds(0, 2 * rows)], waves.at[pl.ds(2 * rows, rows)]
    wide = width // CHUNKS
    tiles = wide // TILE
    heads = wide // HEAD_DIM
    keep = KEPT * HEAD_DIM
    has_next = me < n - 1
    has_prev = me > 0
    groups = n // GROUP
    group = me // GROUP
    role = lax.rem(me, GROUP)
    later = groups - 1 - group
    first = role == 0
    lends = role == 1
    borrows = role == 2
    relays = jnp.logical_and(role == 3, later > 0)
    forwards = jnp.logical_and(lends, later > 0)
    even = lax.rem(me, 2) == 0
    own = pl.ds(rows, rows)
    before = pl.ds(0, rows)

    def seq(target):
        return {"seq": lax.rem(target + n, n)}

    barrier = pltpu.get_barrier_semaphore()

    def greet(target, when):
        @pl.when(when)
        def _():
            pl.semaphore_signal(barrier, inc=1, device_id=seq(target), device_id_type=MESH)

    greet(me + 1, has_next)
    greet(me - 1, has_prev)
    greet(me - 2, borrows)
    greet(me + 2, forwards)
    greet(me - 3, jnp.logical_and(first, group > 0))

    @pl.when(first)
    def _():
        def greet_earlier(j, _):
            pl.semaphore_signal(
                barrier, inc=1, device_id=seq(j * GROUP + 2), device_id_type=MESH
            )
            return 0

        lax.fori_loop(0, group, greet_earlier, 0)

    greeted = has_next.astype(jnp.int32) + has_prev.astype(jnp.int32) + mp - 1
    greeted += jnp.where(borrows, later, 0)
    greeted += (first | relays | forwards).astype(jnp.int32)

    for k in range(1, mp):
        pl.semaphore_signal(
            barrier, inc=1, device_id={"mp": lax.rem(col + k, mp)}, device_id_type=MESH
        )

    def load(source, target, sem):
        pltpu.make_async_copy(source, target, sem).start()

    def landed(buffer, sem):
        pltpu.make_async_copy(buffer, buffer, sem).wait()

    def load_key(c, sem):
        load(key_hbm.at[:, pl.ds(c * wide, wide)], keys.at[c, own], sem)

    last = pl.ds(LENT * wide + keep, wide - keep)
    rest = pl.ds(0, LENT * wide + keep)
    load(query_hbm.at[:, last], query.at[:, last], load_sem.at[6])
    load_key(0, key_sem.at[0])
    load_key(HALF, key_sem.at[1])
    load(stream_hbm, stream, load_sem.at[0])
    load(gain_hbm, gain_ref, load_sem.at[2])
    load(decay_hbm, decay_ref, load_sem.at[2])

    def remote(source, target, send, recv, device):
        return pltpu.make_async_remote_copy(
            src_ref=source,
            dst_ref=target,
            send_sem=send,
            recv_sem=recv,
            device_id=device,
            device_id_type=MESH,
        )

    def to_next(buffer, c, send, recv):
        return remote(
            buffer.at[c, own], buffer.at[c, before], send.at[0], recv.at[c], seq(me + 1)
        )

    def to_relay(buffer, c, slot, send):
        return remote(
            buffer.at[c, own], relayed.at[slot], send.at[0], cross_recv.at[slot], seq(me - 2)
        )

    k_copies = [to_next(keys, c, k_send, k_recv) for c in range(CHUNKS)]
    t_copies = [to_next(ext, c, t_send, t_recv) for c in range(CHUNKS)]
    v_copies = [to_next(values, c, v_send, v_recv) for c in range(CHUNKS)]
    lent_query = remote(
        query.at[:, last], next_query, lend_send.at[0], lend_recv.at[0], seq(me - 1)
    )
    lent_stats = remote(stats, stats_in, lend_send.at[1], lend_recv.at[1], seq(me + 1))
    lent_values = remote(
        lent,
        values.at[LENT, before, pl.ds(keep, wide - keep)],
        lend_send.at[4],
        v_recv.at[CHUNKS],
        seq(me + 1),
    )

    def kept(buffer, send, recv):
        part = pl.ds(0, keep)
        return remote(
            buffer.at[LENT, own, part],
            buffer.at[LENT, before, part],
            send,
            recv.at[LENT],
            seq(me + 1),
        )

    kept_keys = kept(keys, lend_send.at[2], k_recv)
    kept_values = kept(values, lend_send.at[3], v_recv)

    key_relay = [
        later > 1 if c >= HALF else True for c in range(CHUNKS)
    ]
    tail_relay = group == 0
    key_slot = [(c + HALF) % CHUNKS for c in range(CHUNKS)]

    def send_key(c, when=True):
        relay = jnp.logical_and(relays, key_relay[c])
        direct = jnp.logical_and(has_next, jnp.logical_not(relay))
        if c == LENT:
            direct = jnp.logical_and(direct, jnp.logical_not(lends))

            @pl.when(lends)
            def _():
                kept_keys.start()

        @pl.when(jnp.logical_and(relay, when))
        def _():
            to_relay(keys, c, key_slot[c], k_send).start()

        @pl.when(jnp.logical_and(direct, when))
        def _():
            k_copies[c].start()

    def send_tail(c):
        direct = has_next
        if c >= HALF:
            relay = jnp.logical_and(relays, tail_relay)
            direct = jnp.logical_and(has_next, jnp.logical_not(relay))

            @pl.when(relay)
            def _():
                to_relay(ext, c, CHUNKS + c - HALF, t_send).start()

        @pl.when(direct)
        def _():
            t_copies[c].start()

    def pass_on(buffer, c, slot, recv, when):
        @pl.when(jnp.logical_and(forwards, when))
        def _():
            remote(
                buffer.at[c, own], relayed.at[slot], k_send.at[0], cross_recv.at[slot], seq(me + 2)
            ).wait_recv()
            remote(
                relayed.at[slot], buffer.at[c, before], cross_send.at[0], recv.at[c], seq(me + 3)
            ).start()

    def pass_key(c):
        pass_on(keys, c, key_slot[c], k_recv, key_relay[c])

    def pass_tail(c):
        pass_on(ext, c, CHUNKS + c - HALF, t_recv, tail_relay)

    def pass_value():
        pass_on(values, 0, CHUNKS + HALF, v_recv, tail_relay)

    @pl.when(me == 0)
    def _():
        for c in range(CHUNKS):
            keys[c, :rows, :] = jnp.zeros((rows, wide), keys.dtype)
            values[c, :rows, :] = jnp.zeros((rows, wide), values.dtype)
            ext[c, :rows, :] = jnp.zeros((rows, wide), ext.dtype)

    def sum_squares():
        landed(stream, load_sem.at[0])

        def square(i, acc):
            x = stream[:, pl.ds(pl.multiple_of(i * 128, 128), 128)].astype(jnp.float32)
            return acc + x * x

        total = lax.fori_loop(
            0, width // 128, square, jnp.zeros((rows, 128), jnp.float32), unroll=4
        )
        squares[...] = jnp.sum(total.T.reshape(128 // 8, 8, rows), axis=0)

    pl.when(jnp.logical_not(even))(sum_squares)
    pl.semaphore_wait(barrier, greeted)
    origin = group == 0
    late = jnp.logical_and(relays, origin)
    landed(query.at[:, last], load_sem.at[6])

    @pl.when(jnp.logical_and(borrows, jnp.logical_not(origin)))
    def _():
        lent_query.start()

    landed(keys.at[0, own], key_sem.at[0])
    send_key(0, jnp.logical_not(late))
    ahead = jnp.logical_and(relays, later == 1)
    landed(keys.at[HALF, own], key_sem.at[1])
    send_key(HALF, ahead)
    load(waves_hbm, waves, load_sem.at[3])
    load(filt_hbm, filt, load_sem.at[4])
    load(sinner_hbm, sinner, load_sem.at[1])
    others = [c for c in range(1, CHUNKS) if c != HALF]
    for i, c in enumerate(others):
        load_key(c, key_sem.at[2 + i])
    load(souter_hbm, souter, load_sem.at[5])
    load(linner_hbm, linner, load_sem.at[5])
    load(louter_hbm, louter, load_sem.at[5])
    load(query_hbm.at[:, rest], query.at[:, rest], load_sem.at[7])
    pl.when(even)(sum_squares)
    sq_copies = [
        pltpu.make_async_remote_copy(
            src_ref=squares,
            dst_ref=squares_in.at[k - 1],
            send_sem=sq_send.at[k - 1],
            recv_sem=sq_recv.at[k - 1],
            device_id={"mp": lax.rem(col + k, mp)},
            device_id_type=MESH,
        )
        for k in range(1, mp)
    ]
    for copy in sq_copies:
        copy.start()

    landed(vectors, load_sem.at[2])
    step = lax.broadcasted_iota(jnp.int32, (rows, TILE), 0).astype(jnp.float32)

    def powers(i, _):
        cols = pl.ds(pl.multiple_of(i * TILE, TILE), TILE)
        exponent = step * decay_ref[:, cols]
        power[:, cols] = jnp.exp(-exponent)
        inv_power[:, cols] = jnp.exp(exponent)
        return 0

    lax.fori_loop(0, width // TILE, powers, 0)
    landed(waves, load_sem.at[3])
    landed(filt, load_sem.at[4])

    def spectra(i, _):
        cols = pl.ds(pl.multiple_of(i * TILE, TILE), TILE)
        spectrum[:, cols] = dot(fwd[:, :rows], filt[:, cols])
        return 0

    lax.fori_loop(0, width // TILE // 2, spectra, 0)
    landed(sinner, load_sem.at[1])
    total = squares[...]
    for k, copy in enumerate(sq_copies):
        copy.wait_recv()
        total = total + squares_in[k]
    mean_square = jnp.sum(total, axis=0, keepdims=True) / channels
    norm = jnp.broadcast_to(1.0 / jnp.sqrt(mean_square + 0.5), (128, rows)).T
    norm = jnp.concatenate([norm] * (TILE // 128), axis=1)

    for c in range(CHUNKS):

        def short(i, _, c=c):
            cols = pl.ds(pl.multiple_of(c * wide + i * TILE, TILE), TILE)
            x = stream[:, cols].astype(jnp.float32) * gain_ref[:, cols] * norm
            ext[c, own, pl.ds(pl.multiple_of(i * TILE, TILE), TILE)] = (
                sinner[:, cols].astype(jnp.float32) * x
            ).astype(jnp.bfloat16)
            return 0

        lax.fori_loop(0, tiles, short, 0)
        send_tail(c)

    for i, c in enumerate(others):
        landed(keys.at[c, own], key_sem.at[2 + i])
    send_key(0, late)
    for c in range(1, CHUNKS):
        send_key(c, jnp.logical_not(ahead) if c == HALF else True)

    lax.fori_loop(width // TILE // 2, width // TILE, spectra, 0)
    landed(blocks.at[pl.ds(3, 3)], load_sem.at[5])
    row = lax.broadcasted_iota(jnp.int32, (rows, 2 * rows), 0)
    column = lax.broadcasted_iota(jnp.int32, (rows, 2 * rows), 1)
    lower = (jnp.where(column >= rows, column - rows, column) <= row).astype(
        jnp.float32
    ).astype(jnp.bfloat16)

    def state_copy(c, target):
        return remote(
            group_state.at[c],
            states.at[c, group],
            e_send.at[target],
            e_recv.at[c],
            seq(target * GROUP),
        )

    def mix_chunk(c):
        @pl.when(has_prev)
        def _():
            t_copies[c].wait_recv()

        def mix(i, _):
            here = pl.ds(pl.multiple_of(i * TILE, TILE), TILE)
            cols = pl.ds(pl.multiple_of(c * wide + i * TILE, TILE), TILE)
            x = dot(fwd[...], ext[c, :, here])
            x_re, x_im = x[:rows], x[rows:]
            h_re, h_im = spectrum[:rows, cols], spectrum[rows:, cols]
            y = jnp.concatenate(
                [x_re * h_re - x_im * h_im, x_re * h_im + x_im * h_re], axis=0
            ).astype(jnp.bfloat16)
            conv = dot(inv[...], y)
            long_in = (
                linner[:, cols].astype(jnp.float32) * souter[:, cols].astype(jnp.float32) * conv
            ).astype(jnp.bfloat16)
            v = long_in.astype(jnp.float32) * inv_power[:, cols]
            high = v.astype(jnp.bfloat16)
            low = (v - high.astype(jnp.float32)).astype(jnp.bfloat16)
            sums = dot(lower, jnp.concatenate([high, low], axis=0))
            cum[:, cols] = sums
            own_state[c, :, here] = sums[rows - 1 :] * power[rows - 1 :, cols]
            return 0

        lax.fori_loop(0, tiles, mix, 0)

        @pl.when(jnp.logical_not(even))
        def _():
            remote(
                own_state.at[c], member_state.at[c], state_send.at[0], state_recv.at[c], seq(me - 1)
            ).start()

    def rate_of(c):
        return decay_ref[:, pl.ds(c * wide, wide)]

    def pair(c):
        @pl.when(first)
        def _():
            landed(member_state.at[c], state_recv.at[c])
            over = jnp.exp(-rate_of(c) * rows)
            pair_state[c] = own_state[c] * over + member_state[c]
            remote(
                pair_state.at[c], before_state.at[c], cross_send.at[0], cross_recv.at[c], seq(me + 2)
            ).start()

    def collect(c):
        @pl.when(borrows)
        def _():
            landed(member_state.at[c], state_recv.at[c])
            landed(before_state.at[c], cross_recv.at[c])
            over = jnp.exp(-rate_of(c) * rows)
            group_state[c] = (before_state[c] * over + own_state[c]) * over + member_state[c]

            def send_state(target, _):
                state_copy(c, target).start()
                return 0

            lax.fori_loop(group + 1, groups, send_state, 0)

    def spread(c):
        @pl.when(first)
        def _():
            for g in range(1, groups):

                @pl.when(group == g)
                def _(g=g):
                    landed(states.at[c, pl.ds(0, g)], e_recv.at[c])

            over_group = jnp.exp(-rate_of(c) * (rows * GROUP))

            def arrive(j, state):
                return state * over_group + states[c, j]

            state = lax.fori_loop(0, group, arrive, jnp.zeros((1, wide), jnp.float32))
            over = jnp.exp(-rate_of(c) * rows)
            carry_in[c] = state
            next_state[c] = state * over + own_state[c]
            give_next(c)
            across_state[c] = state * jnp.exp(-rate_of(c) * (2 * rows)) + pair_state[c]
            remote(
                across_state.at[c], carry_in.at[c], cross_send.at[1], e_recv.at[c], seq(me + 2)
            ).start()

    def give_next(c):
        remote(
            next_state.at[c], carry_in.at[c], state_send.at[0], state_recv.at[c], seq(me + 1)
        ).start()

    def hand_on(c):
        @pl.when(borrows)
        def _():
            landed(carry_in.at[c], e_recv.at[c])
            next_state[c] = carry_in[c] * jnp.exp(-rate_of(c) * rows) + own_state[c]
            give_next(c)

    def long_chunk(c):
        @pl.when(jnp.logical_not(even))
        def _():
            landed(carry_in.at[c], state_recv.at[c])

        rate = rate_of(c)
        carried = carry_in[c] * jnp.exp(-rate)
        z = 2.0 * rate
        scale = jnp.sqrt(jnp.tanh(0.5 * z) * (1.0 + jnp.exp(-z)))
        for i in range(tiles):
            here = pl.ds(i * TILE, TILE)
            cols = pl.ds(c * wide + i * TILE, TILE)
            part = slice(i * TILE, (i + 1) * TILE)
            conv = (cum[:, cols] + carried[:, part]) * power[:, cols]
            out = (
                louter[:, cols].astype(jnp.float32) * (conv * scale[:, part])
            ).astype(jnp.bfloat16)
            values[c, own, here] = out
            mixed[:, cols] = out

        direct = has_next
        if c == LENT:
            direct = jnp.logical_and(has_next, jnp.logical_not(lends))

            @pl.when(lends)
            def _():
                kept_values.start()

                def lend_values(h, _):
                    here = pl.ds(pl.multiple_of(h * HEAD_DIM, HEAD_DIM), HEAD_DIM)
                    there = pl.ds(pl.multiple_of(keep + h * HEAD_DIM, HEAD_DIM), HEAD_DIM)
                    lent[:, here] = dot_tn(
                        lent_weights[h], values[LENT, own, there]
                    ).astype(jnp.bfloat16)
                    return 0

                lax.fori_loop(0, heads - KEPT, lend_values, 0, unroll=heads - KEPT)
                lent_values.start()

        if c == 0:
            relay = jnp.logical_and(relays, group == 0)
            direct = jnp.logical_and(has_next, jnp.logical_not(relay))

            @pl.when(relay)
            def _():
                to_relay(values, c, CHUNKS + HALF, v_send).start()

        if c == 0:
            direct = jnp.logical_and(direct, jnp.logical_not(held))

        @pl.when(direct)
        def _():
            v_copies[c].start()

    def lend_weights():
        @pl.when(lends)
        def _():
            lent_query.wait_recv()
            stats[...] = jnp.ones(stats.shape, stats.dtype)
            for h in range(heads - KEPT):
                here = pl.ds(h * HEAD_DIM, HEAD_DIM)
                there = pl.ds(keep + h * HEAD_DIM, HEAD_DIM)
                s = dot_nt(keys[LENT, own, there], next_query[:, here]) * HEAD_DIM ** (-0.5)
                top = jnp.max(s, axis=0, keepdims=True)
                e = jnp.exp(s - top)
                total = jnp.sum(e, axis=0, keepdims=True)
                lent_weights[h] = (e * (1.0 / total)).astype(jnp.bfloat16)
                stats[h : h + 1, :] = top
                stats[heads + h : heads + h + 1, :] = total
            lent_stats.start()

    valid = (column <= row + rows) & ((column >= rows) | has_prev)

    def score_chunk(c, when=True, half=None):
        if c == LENT:
            when = jnp.logical_not(borrows)

            @pl.when(borrows)
            def _():
                kept_keys.wait_recv()

        @pl.when(jnp.logical_and(has_prev, when if half != 1 else False))
        def _():
            k_copies[c].wait_recv()

        def score(h, _):
            here = pl.ds(pl.multiple_of(h * HEAD_DIM, HEAD_DIM), HEAD_DIM)
            cols = pl.ds(pl.multiple_of(c * wide + h * HEAD_DIM, HEAD_DIM), HEAD_DIM)
            s = dot_nt(query[:, cols], keys[c, :, here]) * HEAD_DIM ** (-0.5)
            s = jnp.where(valid, s, -1e30)
            e = jnp.exp(s - jnp.max(s, axis=1, keepdims=True))
            e = e * (1.0 / jnp.sum(e, axis=1, keepdims=True))
            weights[c, h] = e.astype(jnp.bfloat16)
            return 0

        start = 2 if half == 1 else 0
        stop = 2 if half == 0 else heads

        def run():
            lax.fori_loop(start, stop, score, 0, unroll=2)

        if when is True:
            run()
        else:
            pl.when(when)(run)
        if c == LENT:

            @pl.when(borrows)
            def _():
                lax.fori_loop(0, KEPT, score, 0, unroll=2)

    def borrow():
        @pl.when(borrows)
        def _():
            upper = lax.broadcasted_iota(
                jnp.int32, (rows, rows), 0
            ) <= lax.broadcasted_iota(jnp.int32, (rows, rows), 1)
            stats[...] = jnp.ones(stats.shape, stats.dtype)
            for h in range(heads - KEPT):
                here = pl.ds(keep + h * HEAD_DIM, HEAD_DIM)
                cols = pl.ds(LENT * wide + keep + h * HEAD_DIM, HEAD_DIM)
                s = dot_nt(keys[LENT, own, here], query[:, cols]) * HEAD_DIM ** (-0.5)
                s = jnp.where(upper, s, -1e30)
                top = jnp.max(s, axis=0, keepdims=True)
                e = jnp.exp(s - top)
                lent_weights[h] = e.astype(jnp.bfloat16)
                stats[h : h + 1, :] = top
                stats[heads + h : heads + h + 1, :] = jnp.sum(e, axis=0, keepdims=True)
            for h in range(heads - KEPT):
                here = pl.ds(keep + h * HEAD_DIM, HEAD_DIM)
                own_part[:, here] = dot_tn(lent_weights[h], values[LENT, own, here])

    def blend():
        @pl.when(borrows)
        def _():
            lent_stats.wait_recv()
            top, total = stats[:heads], stats[heads:]
            top_before, total_before = stats_in[:heads], stats_in[heads:]
            most = jnp.maximum(top, top_before)
            here_scale = jnp.exp(top - most)
            before_scale = jnp.exp(top_before - most) * total_before
            inverse = 1.0 / (total * here_scale + before_scale)
            both = jnp.concatenate([here_scale * inverse, before_scale * inverse], axis=0)
            both = jnp.concatenate(
                [both, jnp.zeros((HEAD_DIM - 2 * heads, rows), jnp.float32)], axis=0
            ).T
            for h in range(heads - KEPT):
                here = pl.ds(keep + h * HEAD_DIM, HEAD_DIM)
                own_part[:, here] = own_part[:, here] * both[:, h : h + 1]
                shares[:, here] = jnp.broadcast_to(
                    both[:, heads + h : heads + h + 1], (rows, HEAD_DIM)
                )

    def attend_chunk(c):
        when = has_prev
        if c == LENT:
            when = jnp.logical_and(has_prev, jnp.logical_not(borrows))

        @pl.when(when)
        def _():
            v_copies[c].wait_recv()

        def gather(h, _):
            here = pl.ds(pl.multiple_of(h * HEAD_DIM, HEAD_DIM), HEAD_DIM)
            cols = pl.ds(pl.multiple_of(c * wide + h * HEAD_DIM, HEAD_DIM), HEAD_DIM)
            attended[:, cols] = dot(weights[c, h], values[c, :, here]).astype(jnp.bfloat16)
            return 0

        def finish():
            lax.fori_loop(0, heads, gather, 0, unroll=8)

        if c < LENT:
            finish()
            return
        pl.when(jnp.logical_not(borrows))(finish)

        @pl.when(borrows)
        def _():
            kept_values.wait_recv()
            lax.fori_loop(0, KEPT, gather, 0, unroll=KEPT)
            lent_values.wait_recv()
            for i in range(keep // TILE, tiles):
                here = pl.ds(i * TILE, TILE)
                cols = pl.ds(c * wide + i * TILE, TILE)
                attended[:, cols] = (
                    own_part[:, here]
                    + shares[:, here] * values[c, before, here].astype(jnp.float32)
                ).astype(jnp.bfloat16)

    mix_chunk(0)
    pair(0)
    pass_tail(2)
    mix_chunk(1)
    pair(1)
    collect(0)

    @pl.when(jnp.logical_and(borrows, origin))
    def _():
        lent_query.start()

    pass_tail(3)
    mix_chunk(2)
    pair(2)
    collect(1)
    landed(query.at[:, rest], load_sem.at[7])
    spread(0)
    mix_chunk(3)
    pair(3)
    collect(2)
    spread(1)
    pass_key(0)
    hand_on(0)
    held = relays & (group > 0)
    long_chunk(0)
    score_chunk(0, jnp.logical_not(first), 0)

    @pl.when(held)
    def _():
        v_copies[0].start()

    score_chunk(0, jnp.logical_not(first), 1)
    collect(3)
    spread(2)
    hand_on(1)
    long_chunk(1)
    pass_key(1)
    pass_key(2)
    hand_on(2)
    long_chunk(2)
    lend_weights()
    pass_key(3)
    score_chunk(1, jnp.logical_not(first))
    spread(3)
    hand_on(3)
    long_chunk(3)
    pass_value()
    score_chunk(0, first)
    score_chunk(1, first)
    score_chunk(2)
    score_chunk(3)
    borrow()
    for c in range(CHUNKS - 1):
        attend_chunk(c)
    blend()
    attend_chunk(LENT)

    for copy in sq_copies:
        copy.wait_send()

    def sent(buffer, sem):
        pltpu.make_async_copy(buffer, buffer, sem).wait()

    @pl.when(jnp.logical_not(even))
    def _():
        sent(own_state, state_send.at[0])

    @pl.when(even)
    def _():
        sent(next_state, state_send.at[0])

    @pl.when(first)
    def _():
        sent(pair_state, cross_send.at[0])
        sent(across_state, cross_send.at[1])

    @pl.when(borrows)
    def _():
        lent_query.wait_send()

        def all_sent(target, _):
            sent(group_state, e_send.at[target])
            return 0

        lax.fori_loop(group + 1, groups, all_sent, 0)

    for tails in (True, False):
        for fewer in (True, False):
            slots = pl.ds(HALF if fewer else 0, CHUNKS + tails * (HALF + 1) - fewer * HALF)

            @pl.when(forwards & (tail_relay == tails) & ((later == 1) == fewer))
            def _(slots=slots):
                sent(relayed.at[slots], cross_send.at[0])

    @pl.when(lends)
    def _():
        sent(keys.at[pl.ds(0, LENT), own], k_send.at[0])
        sent(ext.at[:, own], t_send.at[0])
        sent(values.at[pl.ds(0, LENT), own], v_send.at[0])
        lent_stats.wait_send()
        kept_keys.wait_send()
        kept_values.wait_send()
        lent_values.wait_send()

    @pl.when(jnp.logical_and(has_next, jnp.logical_not(lends)))
    def _():
        sent(keys.at[:, own], k_send.at[0])
        sent(ext.at[:, own], t_send.at[0])
        sent(values.at[:, own], v_send.at[0])


def store(mixed, attended, mixed_hbm, attended_hbm, sem):
    rows = mixed.shape[0]
    parts = [pl.ds(i * rows // STORES, rows // STORES) for i in range(STORES)]
    copies = [
        pltpu.make_async_copy(source.at[part], target.at[part], sem.at[k, i])
        for k, (source, target) in enumerate([(mixed, mixed_hbm), (attended, attended_hbm)])
        for i, part in enumerate(parts)
    ]
    for copy in copies:
        copy.start()
    for copy in copies:
        copy.wait()


def on_device(
    n,
    mp,
    stream,
    norm_gain,
    short_outer,
    short_inner,
    short_filter,
    long_outer,
    long_inner,
    long_decay,
    query_heads,
    key_heads,
):
    rows, width = stream.shape
    wide = width // CHUNKS
    heads = wide // HEAD_DIM
    groups = n // GROUP
    bf16, f32 = jnp.bfloat16, jnp.float32
    anywhere = pl.BlockSpec(memory_space=pltpu.HBM)
    vmem = pl.BlockSpec(memory_space=pltpu.VMEM)
    dma = pltpu.SemaphoreType.DMA

    def in_hbm(array):
        return pltpu.with_memory_space_constraint(array, pltpu.HBM)

    mixed, attended = pl.pallas_call(
        functools.partial(kernel, n, mp, float(width * mp)),
        out_shape=[jax.ShapeDtypeStruct((rows, width), bf16)] * 2,
        in_specs=[anywhere] * 11,
        out_specs=[vmem] * 2,
        scratch_shapes=[
            pltpu.VMEM((2, 1, width), f32),
            pltpu.VMEM((7, rows, width), bf16),
            pltpu.VMEM((3 * rows, 2 * rows), bf16),
        ]
        + [pltpu.VMEM((CHUNKS, 2 * rows, wide), bf16)] * 3
        + [pltpu.VMEM((CHUNKS + HALF + 1, rows, wide), bf16)]
        + [pltpu.VMEM((rows, wide - KEPT * HEAD_DIM), bf16)] * 2
        + [pltpu.VMEM((rows, wide), f32)] * 2
        + [pltpu.VMEM((rows, width), f32)] * 3
        + [
            pltpu.VMEM((2 * rows, width), f32),
            pltpu.VMEM((CHUNKS, heads, rows, 2 * rows), bf16),
            pltpu.VMEM((heads, rows, rows), bf16),
        ]
        + [pltpu.VMEM((2 * heads, rows), f32)] * 2
        + [
            pltpu.VMEM((8, rows), f32),
            pltpu.VMEM((mp - 1, 8, rows), f32),
        ]
        + [pltpu.VMEM((CHUNKS, 1, wide), f32)] * 8
        + [
            pltpu.VMEM((CHUNKS, groups, 1, wide), f32),
            dma((8,)),
            dma((CHUNKS,)),
            dma((mp - 1,)),
            dma((mp - 1,)),
        ]
        + [dma((1,)), dma((CHUNKS,))] * 2
        + [dma((1,)), dma((CHUNKS + 1,))]
        + [dma((2,)), dma((CHUNKS + HALF + 1,))]
        + [dma((1,)), dma((CHUNKS,))]
        + [dma((groups,)), dma((CHUNKS,))]
        + [dma((5,)), dma((2,))],
        compiler_params=pltpu.CompilerParams(
            collective_id=0, has_side_effects=True, vmem_limit_bytes=51 * 1024 * 1024
        ),
    )(
        in_hbm(norm_gain.reshape(1, width)),
        in_hbm(long_decay.reshape(1, width)),
        in_hbm(jnp.asarray(waves_of(rows), bf16)),
        stream,
        short_outer,
        short_inner,
        short_filter,
        long_outer,
        long_inner,
        query_heads,
        key_heads,
    )
    return pl.pallas_call(
        store,
        out_shape=[jax.ShapeDtypeStruct((rows, width), bf16)] * 2,
        in_specs=[vmem] * 2,
        out_specs=[anywhere] * 2,
        scratch_shapes=[dma((2, STORES))],
        compiler_params=pltpu.CompilerParams(vmem_limit_bytes=1024 * 1024),
    )(mixed, attended)


def solution(mesh):
    return jax.shard_map(
        functools.partial(on_device, mesh.shape["seq"], mesh.shape["mp"]),
        mesh=mesh,
        in_specs=(
            P("seq", "mp"),
            P("mp"),
            P("seq", "mp"),
            P("seq", "mp"),
            P(None, "mp"),
            P("seq", "mp"),
            P("seq", "mp"),
            P("mp"),
            P("seq", "mp"),
            P("seq", "mp"),
        ),
        out_specs=(P("seq", "mp"), P("seq", "mp")),
        check_vma=False,
    )
```

```python
import functools

import jax
import jax.numpy as jnp
import numpy as np
from jax import lax
from jax.experimental import pallas as pl
from jax.experimental.pallas import tpu as pltpu
from jax.sharding import PartitionSpec as P

HEAD_DIM = 128
CHUNKS = 4
HALF = CHUNKS // 2
LENT = CHUNKS - 1
KEPT = 2
GROUP = 4
TILE = 256
STORES = 2
MESH = pl.DeviceIdType.MESH


def wave(frequency, place, rows):
    shift = np.where(frequency >= rows, rows, 0)
    index = ((2 * (frequency % rows) + 1) * place + shift) % (4 * rows)
    return np.cos(index * (np.pi / (2 * rows)))


def waves_of(rows):
    every = np.arange(2 * rows)
    fwd = wave(every[:, None], every[None, :], rows)
    inv = wave(every[None, :], every[:rows, None] + rows, rows) / rows
    return np.concatenate([fwd, inv], axis=0)


def dot(a, b):
    return jnp.dot(a, b, preferred_element_type=jnp.float32)


def dot_nt(a, b):
    return lax.dot_general(a, b, (((1,), (1,)), ((), ())), preferred_element_type=jnp.float32)


def dot_tn(a, b):
    return lax.dot_general(a, b, (((0,), (0,)), ((), ())), preferred_element_type=jnp.float32)


def kernel(
    n,
    mp,
    channels,
    gain_hbm,
    decay_hbm,
    waves_hbm,
    stream_hbm,
    souter_hbm,
    sinner_hbm,
    filt_hbm,
    louter_hbm,
    linner_hbm,
    query_hbm,
    key_hbm,
    mixed,
    attended,
    vectors,
    blocks,
    waves,
    keys,
    values,
    ext,
    relayed,
    next_query,
    lent,
    own_part,
    shares,
    power,
    inv_power,
    cum,
    spectrum,
    weights,
    lent_weights,
    stats,
    stats_in,
    squares,
    squares_in,
    own_state,
    member_state,
    pair_state,
    before_state,
    group_state,
    next_state,
    across_state,
    carry_in,
    states,
    load_sem,
    key_sem,
    sq_send,
    sq_recv,
    k_send,
    k_recv,
    t_send,
    t_recv,
    v_send,
    v_recv,
    cross_send,
    cross_recv,
    state_send,
    state_recv,
    e_send,
    e_recv,
    lend_send,
    lend_recv,
):
    gain_ref, decay_ref = vectors.at[0], vectors.at[1]
    stream, sinner, filt, souter, linner, louter, query = (blocks.at[i] for i in range(7))
    me = lax.axis_index("seq")
    col = lax.axis_index("mp")
    rows, width = stream.shape
    fwd, inv = waves.at[pl.ds(0, 2 * rows)], waves.at[pl.ds(2 * rows, rows)]
    wide = width // CHUNKS
    tiles = wide // TILE
    heads = wide // HEAD_DIM
    keep = KEPT * HEAD_DIM
    has_next = me < n - 1
    has_prev = me > 0
    groups = n // GROUP
    group = me // GROUP
    role = lax.rem(me, GROUP)
    later = groups - 1 - group
    first = role == 0
    lends = role == 1
    borrows = role == 2
    relays = jnp.logical_and(role == 3, later > 0)
    forwards = jnp.logical_and(lends, later > 0)
    even = lax.rem(me, 2) == 0
    own = pl.ds(rows, rows)
    before = pl.ds(0, rows)

    def seq(target):
        return {"seq": lax.rem(target + n, n)}

    barrier = pltpu.get_barrier_semaphore()

    def greet(target, when):
        @pl.when(when)
        def _():
            pl.semaphore_signal(barrier, inc=1, device_id=seq(target), device_id_type=MESH)

    greet(me + 1, has_next)
    greet(me - 1, has_prev)
    greet(me - 2, borrows)
    greet(me + 2, forwards)
    greet(me - 3, jnp.logical_and(first, group > 0))

    @pl.when(first)
    def _():
        def greet_earlier(j, _):
            pl.semaphore_signal(
                barrier, inc=1, device_id=seq(j * GROUP + 2), device_id_type=MESH
            )
            return 0

        lax.fori_loop(0, group, greet_earlier, 0)

    greeted = has_next.astype(jnp.int32) + has_prev.astype(jnp.int32) + mp - 1
    greeted += jnp.where(borrows, later, 0)
    greeted += (first | relays | forwards).astype(jnp.int32)

    for k in range(1, mp):
        pl.semaphore_signal(
            barrier, inc=1, device_id={"mp": lax.rem(col + k, mp)}, device_id_type=MESH
        )

    def load(source, target, sem):
        pltpu.make_async_copy(source, target, sem).start()

    def landed(buffer, sem):
        pltpu.make_async_copy(buffer, buffer, sem).wait()

    def load_key(c, sem):
        load(key_hbm.at[:, pl.ds(c * wide, wide)], keys.at[c, own], sem)

    last = pl.ds(LENT * wide + keep, wide - keep)
    rest = pl.ds(0, LENT * wide + keep)
    load(query_hbm.at[:, last], query.at[:, last], load_sem.at[6])
    load_key(0, key_sem.at[0])
    load_key(HALF, key_sem.at[1])
    load(stream_hbm, stream, load_sem.at[0])
    load(gain_hbm, gain_ref, load_sem.at[2])
    load(decay_hbm, decay_ref, load_sem.at[2])

    def remote(source, target, send, recv, device):
        return pltpu.make_async_remote_copy(
            src_ref=source,
            dst_ref=target,
            send_sem=send,
            recv_sem=recv,
            device_id=device,
            device_id_type=MESH,
        )

    def to_next(buffer, c, send, recv):
        return remote(
            buffer.at[c, own], buffer.at[c, before], send.at[0], recv.at[c], seq(me + 1)
        )

    def to_relay(buffer, c, slot, send):
        return remote(
            buffer.at[c, own], relayed.at[slot], send.at[0], cross_recv.at[slot], seq(me - 2)
        )

    k_copies = [to_next(keys, c, k_send, k_recv) for c in range(CHUNKS)]
    t_copies = [to_next(ext, c, t_send, t_recv) for c in range(CHUNKS)]
    v_copies = [to_next(values, c, v_send, v_recv) for c in range(CHUNKS)]
    lent_query = remote(
        query.at[:, last], next_query, lend_send.at[0], lend_recv.at[0], seq(me - 1)
    )
    lent_stats = remote(stats, stats_in, lend_send.at[1], lend_recv.at[1], seq(me + 1))
    lent_values = remote(
        lent,
        values.at[LENT, before, pl.ds(keep, wide - keep)],
        lend_send.at[4],
        v_recv.at[CHUNKS],
        seq(me + 1),
    )

    def kept(buffer, send, recv):
        part = pl.ds(0, keep)
        return remote(
            buffer.at[LENT, own, part],
            buffer.at[LENT, before, part],
            send,
            recv.at[LENT],
            seq(me + 1),
        )

    kept_keys = kept(keys, lend_send.at[2], k_recv)
    kept_values = kept(values, lend_send.at[3], v_recv)

    key_relay = [
        later > 1 if c >= HALF else True for c in range(CHUNKS)
    ]
    tail_relay = group == 0
    key_slot = [(c + HALF) % CHUNKS for c in range(CHUNKS)]

    def send_key(c, when=True):
        relay = jnp.logical_and(relays, key_relay[c])
        direct = jnp.logical_and(has_next, jnp.logical_not(relay))
        if c == LENT:
            direct = jnp.logical_and(direct, jnp.logical_not(lends))

            @pl.when(lends)
            def _():
                kept_keys.start()

        @pl.when(jnp.logical_and(relay, when))
        def _():
            to_relay(keys, c, key_slot[c], k_send).start()

        @pl.when(jnp.logical_and(direct, when))
        def _():
            k_copies[c].start()

    def send_tail(c):
        direct = has_next
        if c >= HALF:
            relay = jnp.logical_and(relays, tail_relay)
            direct = jnp.logical_and(has_next, jnp.logical_not(relay))

            @pl.when(relay)
            def _():
                to_relay(ext, c, CHUNKS + c - HALF, t_send).start()

        @pl.when(direct)
        def _():
            t_copies[c].start()

    def pass_on(buffer, c, slot, recv, when):
        @pl.when(jnp.logical_and(forwards, when))
        def _():
            remote(
                buffer.at[c, own], relayed.at[slot], k_send.at[0], cross_recv.at[slot], seq(me + 2)
            ).wait_recv()
            remote(
                relayed.at[slot], buffer.at[c, before], cross_send.at[0], recv.at[c], seq(me + 3)
            ).start()

    def pass_key(c):
        pass_on(keys, c, key_slot[c], k_recv, key_relay[c])

    def pass_tail(c):
        pass_on(ext, c, CHUNKS + c - HALF, t_recv, tail_relay)

    def pass_value():
        pass_on(values, 0, CHUNKS + HALF, v_recv, tail_relay)

    @pl.when(me == 0)
    def _():
        for c in range(CHUNKS):
            keys[c, :rows, :] = jnp.zeros((rows, wide), keys.dtype)
            values[c, :rows, :] = jnp.zeros((rows, wide), values.dtype)
            ext[c, :rows, :] = jnp.zeros((rows, wide), ext.dtype)

    def sum_squares():
        landed(stream, load_sem.at[0])

        def square(i, acc):
            x = stream[:, pl.ds(pl.multiple_of(i * 128, 128), 128)].astype(jnp.float32)
            return acc + x * x

        total = lax.fori_loop(
            0, width // 128, square, jnp.zeros((rows, 128), jnp.float32), unroll=4
        )
        squares[...] = jnp.sum(total.T.reshape(128 // 8, 8, rows), axis=0)

    pl.when(jnp.logical_not(even))(sum_squares)
    pl.semaphore_wait(barrier, greeted)
    origin = group == 0
    late = jnp.logical_and(relays, origin)
    landed(query.at[:, last], load_sem.at[6])

    @pl.when(jnp.logical_and(borrows, jnp.logical_not(origin)))
    def _():
        lent_query.start()

    landed(keys.at[0, own], key_sem.at[0])
    send_key(0, jnp.logical_not(late))
    ahead = jnp.logical_and(relays, later == 1)
    landed(keys.at[HALF, own], key_sem.at[1])
    send_key(HALF, ahead)
    load(waves_hbm, waves, load_sem.at[3])
    load(filt_hbm, filt, load_sem.at[4])
    load(sinner_hbm, sinner, load_sem.at[1])
    others = [c for c in range(1, CHUNKS) if c != HALF]
    for i, c in enumerate(others):
        load_key(c, key_sem.at[2 + i])
    load(souter_hbm, souter, load_sem.at[5])
    load(linner_hbm, linner, load_sem.at[5])
    load(louter_hbm, louter, load_sem.at[5])
    load(query_hbm.at[:, rest], query.at[:, rest], load_sem.at[7])
    pl.when(even)(sum_squares)
    sq_copies = [
        pltpu.make_async_remote_copy(
            src_ref=squares,
            dst_ref=squares_in.at[k - 1],
            send_sem=sq_send.at[k - 1],
            recv_sem=sq_recv.at[k - 1],
            device_id={"mp": lax.rem(col + k, mp)},
            device_id_type=MESH,
        )
        for k in range(1, mp)
    ]
    for copy in sq_copies:
        copy.start()

    landed(vectors, load_sem.at[2])
    step = lax.broadcasted_iota(jnp.int32, (rows, TILE), 0).astype(jnp.float32)

    def powers(i, _):
        cols = pl.ds(pl.multiple_of(i * TILE, TILE), TILE)
        exponent = step * decay_ref[:, cols]
        power[:, cols] = jnp.exp(-exponent)
        inv_power[:, cols] = jnp.exp(exponent)
        return 0

    lax.fori_loop(0, width // TILE, powers, 0)
    landed(waves, load_sem.at[3])
    landed(filt, load_sem.at[4])

    def spectra(i, _):
        cols = pl.ds(pl.multiple_of(i * TILE, TILE), TILE)
        spectrum[:, cols] = dot(fwd[:, :rows], filt[:, cols])
        return 0

    lax.fori_loop(0, width // TILE // 2, spectra, 0)
    landed(sinner, load_sem.at[1])
    total = squares[...]
    for k, copy in enumerate(sq_copies):
        copy.wait_recv()
        total = total + squares_in[k]
    mean_square = jnp.sum(total, axis=0, keepdims=True) / channels
    norm = jnp.broadcast_to(1.0 / jnp.sqrt(mean_square + 0.5), (128, rows)).T
    norm = jnp.concatenate([norm] * (TILE // 128), axis=1)

    for c in range(CHUNKS):

        def short(i, _, c=c):
            cols = pl.ds(pl.multiple_of(c * wide + i * TILE, TILE), TILE)
            x = stream[:, cols].astype(jnp.float32) * gain_ref[:, cols] * norm
            ext[c, own, pl.ds(pl.multiple_of(i * TILE, TILE), TILE)] = (
                sinner[:, cols].astype(jnp.float32) * x
            ).astype(jnp.bfloat16)
            return 0

        lax.fori_loop(0, tiles, short, 0)
        send_tail(c)

    for i, c in enumerate(others):
        landed(keys.at[c, own], key_sem.at[2 + i])
    send_key(0, late)
    for c in range(1, CHUNKS):
        send_key(c, jnp.logical_not(ahead) if c == HALF else True)

    lax.fori_loop(width // TILE // 2, width // TILE, spectra, 0)
    landed(blocks.at[pl.ds(3, 3)], load_sem.at[5])
    row = lax.broadcasted_iota(jnp.int32, (rows, 2 * rows), 0)
    column = lax.broadcasted_iota(jnp.int32, (rows, 2 * rows), 1)
    lower = (jnp.where(column >= rows, column - rows, column) <= row).astype(
        jnp.float32
    ).astype(jnp.bfloat16)

    def state_copy(c, target):
        return remote(
            group_state.at[c],
            states.at[c, group],
            e_send.at[target],
            e_recv.at[c],
            seq(target * GROUP),
        )

    def mix_chunk(c):
        @pl.when(has_prev)
        def _():
            t_copies[c].wait_recv()

        def mix(i, _):
            here = pl.ds(pl.multiple_of(i * TILE, TILE), TILE)
            cols = pl.ds(pl.multiple_of(c * wide + i * TILE, TILE), TILE)
            x = dot(fwd[...], ext[c, :, here])
            x_re, x_im = x[:rows], x[rows:]
            h_re, h_im = spectrum[:rows, cols], spectrum[rows:, cols]
            y = jnp.concatenate(
                [x_re * h_re - x_im * h_im, x_re * h_im + x_im * h_re], axis=0
            ).astype(jnp.bfloat16)
            conv = dot(inv[...], y)
            long_in = (
                linner[:, cols].astype(jnp.float32) * souter[:, cols].astype(jnp.float32) * conv
            ).astype(jnp.bfloat16)
            v = long_in.astype(jnp.float32) * inv_power[:, cols]
            high = v.astype(jnp.bfloat16)
            low = (v - high.astype(jnp.float32)).astype(jnp.bfloat16)
            sums = dot(lower, jnp.concatenate([high, low], axis=0))
            cum[:, cols] = sums
            own_state[c, :, here] = sums[rows - 1 :] * power[rows - 1 :, cols]
            return 0

        lax.fori_loop(0, tiles, mix, 0)

        @pl.when(jnp.logical_not(even))
        def _():
            remote(
                own_state.at[c], member_state.at[c], state_send.at[0], state_recv.at[c], seq(me - 1)
            ).start()

    def rate_of(c):
        return decay_ref[:, pl.ds(c * wide, wide)]

    def pair(c):
        @pl.when(first)
        def _():
            landed(member_state.at[c], state_recv.at[c])
            over = jnp.exp(-rate_of(c) * rows)
            pair_state[c] = own_state[c] * over + member_state[c]
            remote(
                pair_state.at[c], before_state.at[c], cross_send.at[0], cross_recv.at[c], seq(me + 2)
            ).start()

    def collect(c):
        @pl.when(borrows)
        def _():
            landed(member_state.at[c], state_recv.at[c])
            landed(before_state.at[c], cross_recv.at[c])
            over = jnp.exp(-rate_of(c) * rows)
            group_state[c] = (before_state[c] * over + own_state[c]) * over + member_state[c]

            def send_state(target, _):
                state_copy(c, target).start()
                return 0

            lax.fori_loop(group + 1, groups, send_state, 0)

    def spread(c):
        @pl.when(first)
        def _():
            for g in range(1, groups):

                @pl.when(group == g)
                def _(g=g):
                    landed(states.at[c, pl.ds(0, g)], e_recv.at[c])

            over_group = jnp.exp(-rate_of(c) * (rows * GROUP))

            def arrive(j, state):
                return state * over_group + states[c, j]

            state = lax.fori_loop(0, group, arrive, jnp.zeros((1, wide), jnp.float32))
            over = jnp.exp(-rate_of(c) * rows)
            carry_in[c] = state
            next_state[c] = state * over + own_state[c]
            give_next(c)
            across_state[c] = state * jnp.exp(-rate_of(c) * (2 * rows)) + pair_state[c]
            remote(
                across_state.at[c], carry_in.at[c], cross_send.at[1], e_recv.at[c], seq(me + 2)
            ).start()

    def give_next(c):
        remote(
            next_state.at[c], carry_in.at[c], state_send.at[0], state_recv.at[c], seq(me + 1)
        ).start()

    def hand_on(c):
        @pl.when(borrows)
        def _():
            landed(carry_in.at[c], e_recv.at[c])
            next_state[c] = carry_in[c] * jnp.exp(-rate_of(c) * rows) + own_state[c]
            give_next(c)

    def long_chunk(c):
        @pl.when(jnp.logical_not(even))
        def _():
            landed(carry_in.at[c], state_recv.at[c])

        rate = rate_of(c)
        carried = carry_in[c] * jnp.exp(-rate)
        z = 2.0 * rate
        scale = jnp.sqrt(jnp.tanh(0.5 * z) * (1.0 + jnp.exp(-z)))
        for i in range(tiles):
            here = pl.ds(i * TILE, TILE)
            cols = pl.ds(c * wide + i * TILE, TILE)
            part = slice(i * TILE, (i + 1) * TILE)
            conv = (cum[:, cols] + carried[:, part]) * power[:, cols]
            out = (
                louter[:, cols].astype(jnp.float32) * (conv * scale[:, part])
            ).astype(jnp.bfloat16)
            values[c, own, here] = out
            mixed[:, cols] = out

        direct = has_next
        if c == LENT:
            direct = jnp.logical_and(has_next, jnp.logical_not(lends))

            @pl.when(lends)
            def _():
                kept_values.start()

                def lend_values(h, _):
                    here = pl.ds(pl.multiple_of(h * HEAD_DIM, HEAD_DIM), HEAD_DIM)
                    there = pl.ds(pl.multiple_of(keep + h * HEAD_DIM, HEAD_DIM), HEAD_DIM)
                    lent[:, here] = dot_tn(
                        lent_weights[h], values[LENT, own, there]
                    ).astype(jnp.bfloat16)
                    return 0

                lax.fori_loop(0, heads - KEPT, lend_values, 0, unroll=heads - KEPT)
                lent_values.start()

        if c == 0:
            relay = jnp.logical_and(relays, group == 0)
            direct = jnp.logical_and(has_next, jnp.logical_not(relay))

            @pl.when(relay)
            def _():
                to_relay(values, c, CHUNKS + HALF, v_send).start()

        if c == 0:
            direct = jnp.logical_and(direct, jnp.logical_not(held))

        @pl.when(direct)
        def _():
            v_copies[c].start()

    def lend_weights():
        @pl.when(lends)
        def _():
            lent_query.wait_recv()
            stats[...] = jnp.ones(stats.shape, stats.dtype)
            for h in range(heads - KEPT):
                here = pl.ds(h * HEAD_DIM, HEAD_DIM)
                there = pl.ds(keep + h * HEAD_DIM, HEAD_DIM)
                s = dot_nt(keys[LENT, own, there], next_query[:, here]) * HEAD_DIM ** (-0.5)
                top = jnp.max(s, axis=0, keepdims=True)
                e = jnp.exp(s - top)
                total = jnp.sum(e, axis=0, keepdims=True)
                lent_weights[h] = (e * (1.0 / total)).astype(jnp.bfloat16)
                stats[h : h + 1, :] = top
                stats[heads + h : heads + h + 1, :] = total
            lent_stats.start()

    valid = (column <= row + rows) & ((column >= rows) | has_prev)

    def score_chunk(c, when=True, half=None):
        if c == LENT:
            when = jnp.logical_not(borrows)

            @pl.when(borrows)
            def _():
                kept_keys.wait_recv()

        @pl.when(jnp.logical_and(has_prev, when if half != 1 else False))
        def _():
            k_copies[c].wait_recv()

        def score(h, _):
            here = pl.ds(pl.multiple_of(h * HEAD_DIM, HEAD_DIM), HEAD_DIM)
            cols = pl.ds(pl.multiple_of(c * wide + h * HEAD_DIM, HEAD_DIM), HEAD_DIM)
            s = dot_nt(query[:, cols], keys[c, :, here]) * HEAD_DIM ** (-0.5)
            s = jnp.where(valid, s, -1e30)
            e = jnp.exp(s - jnp.max(s, axis=1, keepdims=True))
            e = e * (1.0 / jnp.sum(e, axis=1, keepdims=True))
            weights[c, h] = e.astype(jnp.bfloat16)
            return 0

        start = 2 if half == 1 else 0
        stop = 2 if half == 0 else heads

        def run():
            lax.fori_loop(start, stop, score, 0, unroll=2)

        if when is True:
            run()
        else:
            pl.when(when)(run)
        if c == LENT:

            @pl.when(borrows)
            def _():
                lax.fori_loop(0, KEPT, score, 0, unroll=2)

    def borrow():
        @pl.when(borrows)
        def _():
            upper = lax.broadcasted_iota(
                jnp.int32, (rows, rows), 0
            ) <= lax.broadcasted_iota(jnp.int32, (rows, rows), 1)
            stats[...] = jnp.ones(stats.shape, stats.dtype)
            for h in range(heads - KEPT):
                here = pl.ds(keep + h * HEAD_DIM, HEAD_DIM)
                cols = pl.ds(LENT * wide + keep + h * HEAD_DIM, HEAD_DIM)
                s = dot_nt(keys[LENT, own, here], query[:, cols]) * HEAD_DIM ** (-0.5)
                s = jnp.where(upper, s, -1e30)
                top = jnp.max(s, axis=0, keepdims=True)
                e = jnp.exp(s - top)
                lent_weights[h] = e.astype(jnp.bfloat16)
                stats[h : h + 1, :] = top
                stats[heads + h : heads + h + 1, :] = jnp.sum(e, axis=0, keepdims=True)
            for h in range(heads - KEPT):
                here = pl.ds(keep + h * HEAD_DIM, HEAD_DIM)
                own_part[:, here] = dot_tn(lent_weights[h], values[LENT, own, here])

    def blend():
        @pl.when(borrows)
        def _():
            lent_stats.wait_recv()
            top, total = stats[:heads], stats[heads:]
            top_before, total_before = stats_in[:heads], stats_in[heads:]
            most = jnp.maximum(top, top_before)
            here_scale = jnp.exp(top - most)
            before_scale = jnp.exp(top_before - most) * total_before
            inverse = 1.0 / (total * here_scale + before_scale)
            both = jnp.concatenate([here_scale * inverse, before_scale * inverse], axis=0)
            both = jnp.concatenate(
                [both, jnp.zeros((HEAD_DIM - 2 * heads, rows), jnp.float32)], axis=0
            ).T
            for h in range(heads - KEPT):
                here = pl.ds(keep + h * HEAD_DIM, HEAD_DIM)
                own_part[:, here] = own_part[:, here] * both[:, h : h + 1]
                shares[:, here] = jnp.broadcast_to(
                    both[:, heads + h : heads + h + 1], (rows, HEAD_DIM)
                )

    def attend_chunk(c):
        when = has_prev
        if c == LENT:
            when = jnp.logical_and(has_prev, jnp.logical_not(borrows))

        @pl.when(when)
        def _():
            v_copies[c].wait_recv()

        def gather(h, _):
            here = pl.ds(pl.multiple_of(h * HEAD_DIM, HEAD_DIM), HEAD_DIM)
            cols = pl.ds(pl.multiple_of(c * wide + h * HEAD_DIM, HEAD_DIM), HEAD_DIM)
            attended[:, cols] = dot(weights[c, h], values[c, :, here]).astype(jnp.bfloat16)
            return 0

        def finish():
            lax.fori_loop(0, heads, gather, 0, unroll=8)

        if c < LENT:
            finish()
            return
        pl.when(jnp.logical_not(borrows))(finish)

        @pl.when(borrows)
        def _():
            kept_values.wait_recv()
            lax.fori_loop(0, KEPT, gather, 0, unroll=KEPT)
            lent_values.wait_recv()
            for i in range(keep // TILE, tiles):
                here = pl.ds(i * TILE, TILE)
                cols = pl.ds(c * wide + i * TILE, TILE)
                attended[:, cols] = (
                    own_part[:, here]
                    + shares[:, here] * values[c, before, here].astype(jnp.float32)
                ).astype(jnp.bfloat16)

    mix_chunk(0)
    pair(0)
    pass_tail(2)
    mix_chunk(1)
    pair(1)
    collect(0)

    @pl.when(jnp.logical_and(borrows, origin))
    def _():
        lent_query.start()

    pass_tail(3)
    mix_chunk(2)
    pair(2)
    collect(1)
    landed(query.at[:, rest], load_sem.at[7])
    spread(0)
    mix_chunk(3)
    pair(3)
    collect(2)
    spread(1)
    pass_key(0)
    hand_on(0)
    held = relays & (group > 0) & (later > 1)
    long_chunk(0)
    score_chunk(0, jnp.logical_not(first), 0)

    @pl.when(held)
    def _():
        v_copies[0].start()

    score_chunk(0, jnp.logical_not(first), 1)
    collect(3)
    spread(2)
    hand_on(1)
    long_chunk(1)
    pass_key(1)
    pass_key(2)
    hand_on(2)
    long_chunk(2)
    lend_weights()
    pass_key(3)
    score_chunk(1, jnp.logical_not(first))
    spread(3)
    hand_on(3)
    long_chunk(3)
    pass_value()
    score_chunk(0, first)
    score_chunk(1, first)
    score_chunk(2)
    score_chunk(3)
    borrow()
    for c in range(CHUNKS - 1):
        attend_chunk(c)
    blend()
    attend_chunk(LENT)

    for copy in sq_copies:
        copy.wait_send()

    def sent(buffer, sem):
        pltpu.make_async_copy(buffer, buffer, sem).wait()

    @pl.when(jnp.logical_not(even))
    def _():
        sent(own_state, state_send.at[0])

    @pl.when(even)
    def _():
        sent(next_state, state_send.at[0])

    @pl.when(first)
    def _():
        sent(pair_state, cross_send.at[0])
        sent(across_state, cross_send.at[1])

    @pl.when(borrows)
    def _():
        lent_query.wait_send()

        def all_sent(target, _):
            sent(group_state, e_send.at[target])
            return 0

        lax.fori_loop(group + 1, groups, all_sent, 0)

    for tails in (True, False):
        for fewer in (True, False):
            slots = pl.ds(HALF if fewer else 0, CHUNKS + tails * (HALF + 1) - fewer * HALF)

            @pl.when(forwards & (tail_relay == tails) & ((later == 1) == fewer))
            def _(slots=slots):
                sent(relayed.at[slots], cross_send.at[0])

    @pl.when(lends)
    def _():
        sent(keys.at[pl.ds(0, LENT), own], k_send.at[0])
        sent(ext.at[:, own], t_send.at[0])
        sent(values.at[pl.ds(0, LENT), own], v_send.at[0])
        lent_stats.wait_send()
        kept_keys.wait_send()
        kept_values.wait_send()
        lent_values.wait_send()

    @pl.when(jnp.logical_and(has_next, jnp.logical_not(lends)))
    def _():
        sent(keys.at[:, own], k_send.at[0])
        sent(ext.at[:, own], t_send.at[0])
        sent(values.at[:, own], v_send.at[0])


def store(mixed, attended, mixed_hbm, attended_hbm, sem):
    rows = mixed.shape[0]
    parts = [pl.ds(i * rows // STORES, rows // STORES) for i in range(STORES)]
    copies = [
        pltpu.make_async_copy(source.at[part], target.at[part], sem.at[k, i])
        for k, (source, target) in enumerate([(mixed, mixed_hbm), (attended, attended_hbm)])
        for i, part in enumerate(parts)
    ]
    for copy in copies:
        copy.start()
    for copy in copies:
        copy.wait()


def on_device(
    n,
    mp,
    stream,
    norm_gain,
    short_outer,
    short_inner,
    short_filter,
    long_outer,
    long_inner,
    long_decay,
    query_heads,
    key_heads,
):
    rows, width = stream.shape
    wide = width // CHUNKS
    heads = wide // HEAD_DIM
    groups = n // GROUP
    bf16, f32 = jnp.bfloat16, jnp.float32
    anywhere = pl.BlockSpec(memory_space=pltpu.HBM)
    vmem = pl.BlockSpec(memory_space=pltpu.VMEM)
    dma = pltpu.SemaphoreType.DMA

    def in_hbm(array):
        return pltpu.with_memory_space_constraint(array, pltpu.HBM)

    mixed, attended = pl.pallas_call(
        functools.partial(kernel, n, mp, float(width * mp)),
        out_shape=[jax.ShapeDtypeStruct((rows, width), bf16)] * 2,
        in_specs=[anywhere] * 11,
        out_specs=[vmem] * 2,
        scratch_shapes=[
            pltpu.VMEM((2, 1, width), f32),
            pltpu.VMEM((7, rows, width), bf16),
            pltpu.VMEM((3 * rows, 2 * rows), bf16),
        ]
        + [pltpu.VMEM((CHUNKS, 2 * rows, wide), bf16)] * 3
        + [pltpu.VMEM((CHUNKS + HALF + 1, rows, wide), bf16)]
        + [pltpu.VMEM((rows, wide - KEPT * HEAD_DIM), bf16)] * 2
        + [pltpu.VMEM((rows, wide), f32)] * 2
        + [pltpu.VMEM((rows, width), f32)] * 3
        + [
            pltpu.VMEM((2 * rows, width), f32),
            pltpu.VMEM((CHUNKS, heads, rows, 2 * rows), bf16),
            pltpu.VMEM((heads, rows, rows), bf16),
        ]
        + [pltpu.VMEM((2 * heads, rows), f32)] * 2
        + [
            pltpu.VMEM((8, rows), f32),
            pltpu.VMEM((mp - 1, 8, rows), f32),
        ]
        + [pltpu.VMEM((CHUNKS, 1, wide), f32)] * 8
        + [
            pltpu.VMEM((CHUNKS, groups, 1, wide), f32),
            dma((8,)),
            dma((CHUNKS,)),
            dma((mp - 1,)),
            dma((mp - 1,)),
        ]
        + [dma((1,)), dma((CHUNKS,))] * 2
        + [dma((1,)), dma((CHUNKS + 1,))]
        + [dma((2,)), dma((CHUNKS + HALF + 1,))]
        + [dma((1,)), dma((CHUNKS,))]
        + [dma((groups,)), dma((CHUNKS,))]
        + [dma((5,)), dma((2,))],
        compiler_params=pltpu.CompilerParams(
            collective_id=0, has_side_effects=True, vmem_limit_bytes=51 * 1024 * 1024
        ),
    )(
        in_hbm(norm_gain.reshape(1, width)),
        in_hbm(long_decay.reshape(1, width)),
        in_hbm(jnp.asarray(waves_of(rows), bf16)),
        stream,
        short_outer,
        short_inner,
        short_filter,
        long_outer,
        long_inner,
        query_heads,
        key_heads,
    )
    return pl.pallas_call(
        store,
        out_shape=[jax.ShapeDtypeStruct((rows, width), bf16)] * 2,
        in_specs=[vmem] * 2,
        out_specs=[anywhere] * 2,
        scratch_shapes=[dma((2, STORES))],
        compiler_params=pltpu.CompilerParams(vmem_limit_bytes=1024 * 1024),
    )(mixed, attended)


def solution(mesh):
    return jax.shard_map(
        functools.partial(on_device, mesh.shape["seq"], mesh.shape["mp"]),
        mesh=mesh,
        in_specs=(
            P("seq", "mp"),
            P("mp"),
            P("seq", "mp"),
            P("seq", "mp"),
            P(None, "mp"),
            P("seq", "mp"),
            P("seq", "mp"),
            P("mp"),
            P("seq", "mp"),
            P("seq", "mp"),
        ),
        out_specs=(P("seq", "mp"), P("seq", "mp")),
        check_vma=False,
    )
```
